8 devices in a mesh: tp: 4 (over z, y, x), cp: 2 (over core).
Axes of the slice: x: 2, y: 2, z: 1, core: 2. Of those that a mesh axis runs over, the one named last changes fastest.
Arguments:
- x_in: bfloat16 [32, 256, 4096], P(None, 'cp')
- grad_z: bfloat16 [32, 256, 4096], P(None, 'cp')
- seg_pos: int32 [32, 256], P(None, 'cp')
- norm_scale: bfloat16 [4096], replicated
- w_x: bfloat16 [4096, 4096], P(None, 'tp')
- b_x: bfloat16 [4096], P('tp')
- w_y: bfloat16 [4096, 4096], P(None, 'tp')
- b_y: bfloat16 [4096], P('tp')
- conv_w: bfloat16 [4, 4096], P(None, 'tp')
- conv_b: bfloat16 [4096], P('tp')
- w_a: bfloat16 [16, 256, 256], P('tp')
- b_a: bfloat16 [4096], P('tp')
- w_i: bfloat16 [16, 256, 256], P('tp')
- b_i: bfloat16 [4096], P('tp')
- a_param: float32 [4096], P('tp')
- w_out: bfloat16 [4096, 4096], P('tp')
- b_out: bfloat16 [4096], replicated
Outputs:
- output 1: bfloat16 [32, 256, 4096], P(None, 'cp')
- output 2: bfloat16 [32, 256, 4096], P(None, 'cp')
- output 3: float32 [4096], replicated
- output 4: float32 [4096, 4096], P(None, 'tp')
- output 5: float32 [4096], P('tp')
- output 6: float32 [4096, 4096], P(None, 'tp')
- output 7: float32 [4096], P('tp')
- output 8: float32 [4, 4096], P(None, 'tp')
- output 9: float32 [4096], P('tp')
- output 10: float32 [16, 256, 256], P('tp')
- output 11: float32 [4096], P('tp')
- output 12: float32 [16, 256, 256], P('tp')
- output 13: float32 [4096], P('tp')
- output 14: float32 [4096], P('tp')
- output 15: float32 [4096, 4096], P('tp')
- output 16: float32 [4096], replicated
All inputs are finite; a program needn't handle non-finite values.
Results may differ from the reference program's by a relative error of at most 0.00874371.
Values sent between devices are 32-bit elements.
A program may use at most 1 GiB of HBM per device.

```python
import math
import jax
import jax.numpy as jnp
from jax import lax

BATCH_SEQS = 32
SEQ_LEN = 256
D_MODEL = 4096
D_RNN = 4096
GATE_BLOCKS = 16
DOC_STARTS = 2
CONV_WIDTH = 4
BLOCK_WIDTH = D_RNN // GATE_BLOCKS
NORM_EPS = 1e-6


def doc_positions(pos_key):
    starts = jax.random.randint(pos_key, (BATCH_SEQS, DOC_STARTS), 1, SEQ_LEN)
    step_ids = jnp.arange(SEQ_LEN, dtype=jnp.int32)
    is_start = jnp.any(step_ids[None, :, None] == starts[:, None, :], axis=-1) | (step_ids == 0)[None, :]
    last_start = lax.cummax(jnp.where(is_start, step_ids[None, :], 0), axis=1)
    return (step_ids[None, :] - last_start).astype(jnp.int32)


def setup_inputs(seed: int = 0) -> dict:
    key_list = jax.random.split(jax.random.key(seed), 17)

    def draw_normal(key_index, arr_shape, factor):
        return jax.random.normal(key_list[key_index], arr_shape, jnp.float32) * factor

    tok_shape = (BATCH_SEQS, SEQ_LEN, D_MODEL)
    gate_shape = (GATE_BLOCKS, BLOCK_WIDTH, BLOCK_WIDTH)
    soft_plus = jnp.exp(jax.random.uniform(key_list[14], (D_RNN,), jnp.float32, math.log(2e-5), math.log(2e-4)))
    return {
        "x_in": draw_normal(0, tok_shape, 1.0).astype(jnp.bfloat16),
        "grad_z": draw_normal(1, tok_shape, 1.0).astype(jnp.bfloat16),
        "seg_pos": doc_positions(key_list[2]),
        "norm_scale": draw_normal(3, (D_MODEL,), 0.3).astype(jnp.bfloat16),
        "w_x": draw_normal(4, (D_MODEL, D_RNN), D_MODEL ** -0.5).astype(jnp.bfloat16),
        "b_x": draw_normal(5, (D_RNN,), 0.3).astype(jnp.bfloat16),
        "w_y": draw_normal(6, (D_MODEL, D_RNN), D_MODEL ** -0.5).astype(jnp.bfloat16),
        "b_y": draw_normal(7, (D_RNN,), 0.3).astype(jnp.bfloat16),
        "conv_w": draw_normal(8, (CONV_WIDTH, D_RNN), 0.5).astype(jnp.bfloat16),
        "conv_b": draw_normal(9, (D_RNN,), 0.3).astype(jnp.bfloat16),
        "w_a": draw_normal(10, gate_shape, BLOCK_WIDTH ** -0.5).astype(jnp.bfloat16),
        "b_a": draw_normal(11, (D_RNN,), 0.5).astype(jnp.bfloat16),
        "w_i": draw_normal(12, gate_shape, BLOCK_WIDTH ** -0.5).astype(jnp.bfloat16),
        "b_i": draw_normal(13, (D_RNN,), 0.5).astype(jnp.bfloat16),
        "a_param": jnp.log(jnp.expm1(soft_plus)),
        "w_out": draw_normal(15, (D_RNN, D_MODEL), D_RNN ** -0.5).astype(jnp.bfloat16),
        "b_out": draw_normal(16, (D_MODEL,), 0.3).astype(jnp.bfloat16),
    }


def to_bf16(arr_val):
    return arr_val + lax.stop_gradient(arr_val.astype(jnp.bfloat16).astype(jnp.float32) - arr_val)


def block_forward(x_f, norm_scale, w_x, b_x, w_y, b_y, conv_w, conv_b, w_a, b_a, w_i, b_i, a_param, w_out, b_out, seg_pos):
    mean_sq = jnp.mean(x_f * x_f, axis=-1, keepdims=True)
    normed = to_bf16(x_f * lax.rsqrt(mean_sq + NORM_EPS) * (1.0 + norm_scale))
    y_act = jax.nn.gelu(jnp.dot(normed, w_y, preferred_element_type=jnp.float32) + b_y, approximate=True)
    x_branch = to_bf16(jnp.dot(normed, w_x, preferred_element_type=jnp.float32) + b_x)
    batch_n, seq_n, width_n = x_branch.shape
    conv_sum = x_branch * conv_w[0] + conv_b
    for tap_k in range(1, CONV_WIDTH):
        shifted = jnp.pad(x_branch[:, :seq_n - tap_k], ((0, 0), (tap_k, 0), (0, 0)))
        keep_mask = (seg_pos >= tap_k)[:, :, None]
        conv_sum = conv_sum + jnp.where(keep_mask, shifted, 0.0) * conv_w[tap_k]
    conv_out = to_bf16(conv_sum)
    blocks = conv_out.reshape(batch_n, seq_n, GATE_BLOCKS, BLOCK_WIDTH)
    pre_a = jnp.einsum("bthk,hkj->bthj", blocks, w_a).reshape(batch_n, seq_n, width_n) + b_a
    pre_i = jnp.einsum("bthk,hkj->bthj", blocks, w_i).reshape(batch_n, seq_n, width_n) + b_i
    reset_mask = (seg_pos == 0)[:, :, None]
    log_a = -8.0 * jax.nn.sigmoid(pre_a) * jax.nn.softplus(a_param)
    decays = jnp.where(reset_mask, 0.0, jnp.exp(log_a))
    multiplier = jnp.where(reset_mask, 1.0, jnp.sqrt(-jnp.expm1(2.0 * log_a)))
    drives = multiplier * jax.nn.sigmoid(pre_i) * conv_out

    def scan_step(carry_h, inputs_t):
        next_h = inputs_t[0] * carry_h + inputs_t[1]
        return next_h, next_h

    init_h = jnp.zeros((batch_n, width_n), jnp.float32)
    _, hidden_t = lax.scan(scan_step, init_h, (jnp.swapaxes(decays, 0, 1), jnp.swapaxes(drives, 0, 1)))
    hidden = jnp.swapaxes(hidden_t, 0, 1)
    mixed_v = to_bf16(hidden * y_act)
    out_proj = jnp.dot(mixed_v, w_out, preferred_element_type=jnp.float32) + b_out
    return to_bf16(x_f + out_proj)


def reference(x_in, grad_z, seg_pos, norm_scale, w_x, b_x, w_y, b_y, conv_w, conv_b, w_a, b_a, w_i, b_i, a_param, w_out, b_out):
    primals = [param_arr.astype(jnp.float32) for param_arr in (x_in, norm_scale, w_x, b_x, w_y, b_y, conv_w, conv_b, w_a, b_a, w_i, b_i, a_param, w_out, b_out)]

    def run_block(*params):
        return block_forward(*params, seg_pos)

    z_val, pull_back = jax.vjp(run_block, *primals)
    grad_list = pull_back(grad_z.astype(jnp.float32))
    return (z_val.astype(jnp.bfloat16), grad_list[0].astype(jnp.bfloat16), grad_list[1], grad_list[2], grad_list[3], grad_list[4], grad_list[5], grad_list[6], grad_list[7], grad_list[8], grad_list[9], grad_list[10], grad_list[11], grad_list[12], grad_list[13], grad_list[14])
```

```python
import functools
import jax
import jax.numpy as jnp
from jax import lax
from jax.experimental import pallas as pl
from jax.experimental.pallas import tpu as pltpu
from jax.sharding import PartitionSpec as P

NORM_EPS = 1e-6
TINY, FAR = 1e-37, 1e4
LOG2E = 1.4426950408889634
GELU_K0 = 0.7978845608028654
GELU_K1 = GELU_K0 * 0.044715
SUB = 8
TOK, GRP, CH, DM, LANES, TILE = 128, 4, 256, 4096, 128, 16
GROWS = TOK * SUB
ROWS = GRP * GROWS
HALF = DM // 2
PIECE, HALO = 256, 32
KSTEP, STRIP = 1024, 32
POS_ROWS = GROWS + 64
COLS = DM // LANES
BF, F32 = jnp.bfloat16, jnp.float32
ANY = pl.BlockSpec(memory_space=pl.ANY)
VM = pl.BlockSpec(memory_space=pltpu.VMEM)
VMEM_MOST = 67000000
NT = (((1,), (1,)), ((), ()))
TN = (((0,), (0,)), ((), ()))
SEQ, ALL, CHAN, COL, BLK, ROW = P(None, "cp", None), P(), P("tp"), P(None, "tp"), P("tp", None, None), P("tp", None)
PARAMS = (COL, CHAN, COL, CHAN, COL, CHAN, BLK, CHAN, BLK, CHAN, CHAN, ROW, ALL)
IN_SPECS = (SEQ, SEQ, P(None, "cp"), ALL) + PARAMS
OUT_SPECS = (SEQ, SEQ, ALL) + PARAMS


def sds(shape, dtype):
    return jax.ShapeDtypeStruct(shape, dtype)


TOKEN = sds((SUB, LANES), F32)


def cost(us):
    return pl.CostEstimate(flops=int(us * 1e9), bytes_accessed=int(us * 1e6), transcendentals=0)


def params(**kw):
    return pltpu.CompilerParams(vmem_limit_bytes=VMEM_MOST, **kw)


def lane_tiles():
    return [(j, slice(j * LANES, (j + 1) * LANES)) for j in range(COLS)]


NTOK = TOK // TILE
SEQ_BLOCK = pl.BlockSpec((SUB, TILE, DM), lambda g, t: (g, t, 0))
ROW_BLOCK = pl.BlockSpec((SUB * TILE, DM), lambda g, t: (g * NTOK + t, 0))
ONE_ROW = pl.BlockSpec((1, DM), lambda g, t: (0, 0))
SUM_BLOCK = pl.BlockSpec((SUB, DM), lambda g, t: (0, 0))
TURN = pltpu.VMEM((COLS, SUB * TILE, LANES), F32)


def row_call(kernel, us, inputs, in_specs, out_specs, out_shape, turns):
    return pl.pallas_call(kernel, grid=(GRP, NTOK), in_specs=in_specs, out_specs=out_specs, out_shape=out_shape, scratch_shapes=[TURN] * turns,
                          compiler_params=params(), cost_estimate=cost(us))(*inputs)


def first_step():
    return (pl.program_id(0) == 0) & (pl.program_id(1) == 0)


def both(val):
    return val[:SUB] + val[SUB:]


def row_scales(x_ref, more=None):
    found = []
    for b in range(SUB):
        square = other = jnp.zeros((TILE, LANES), F32)
        for j, cols in lane_tiles():
            xf = x_ref[b, :, cols].astype(F32)
            square = square + xf * xf
            if more is not None:
                other = other + xf * more(b, j, cols)
        rstd = lax.rsqrt(jnp.sum(square, axis=-1, keepdims=True) * (1.0 / DM) + NORM_EPS)
        found.append((rstd, jnp.sum(other, axis=-1, keepdims=True) * (1.0 / DM)))
    return found


def norm_kernel(x_ref, gz_ref, sc_ref, n_ref, g_ref, gb_ref, sn_ref, sg_ref):
    @pl.when(first_step())
    def _():
        gb_ref[...] = jnp.zeros_like(gb_ref)

    rows = row_scales(x_ref)
    for j, cols in lane_tiles():
        scale = 1.0 + sc_ref[:, cols]
        total = gb_ref[:, cols]
        for b in range(SUB):
            gf = gz_ref[b, :, cols].astype(F32)
            total = total + both(gf)
            sn_ref[j, pl.ds(b, TILE, stride=SUB), :] = x_ref[b, :, cols].astype(F32) * rows[b][0] * scale
            sg_ref[j, pl.ds(b, TILE, stride=SUB), :] = gf
        gb_ref[:, cols] = total
        n_ref[:, cols] = sn_ref[j].astype(BF)
        g_ref[:, cols] = sg_ref[j].astype(BF)


def norm_call(x, gz, scale):
    return row_call(norm_kernel, 60, (x, gz, scale), [SEQ_BLOCK, SEQ_BLOCK, ONE_ROW], [ROW_BLOCK, ROW_BLOCK, SUM_BLOCK],
                    [sds((ROWS, DM), BF), sds((ROWS, DM), BF), sds((SUB, DM), F32)], 2)


def z_kernel(acc_ref, x_ref, bo_ref, z_ref, sa_ref):
    for j, cols in lane_tiles():
        sa_ref[j] = acc_ref[:, cols]
    for b in range(SUB):
        for j, cols in lane_tiles():
            z_ref[b, :, cols] = (x_ref[b, :, cols].astype(F32) + (sa_ref[j, pl.ds(b, TILE, stride=SUB), :] + bo_ref[:, cols])).astype(BF)


def z_call(acc, x, b_out):
    return row_call(z_kernel, 50, (acc, x, b_out), [ROW_BLOCK, SEQ_BLOCK, ONE_ROW], SEQ_BLOCK, sds((GRP * SUB, TOK, DM), BF), 1)


def gx_kernel(dn_ref, x_ref, gz_ref, sc_ref, gx_ref, gs_ref, sa_ref):
    @pl.when(first_step())
    def _():
        gs_ref[...] = jnp.zeros_like(gs_ref)

    for j, cols in lane_tiles():
        sa_ref[j] = dn_ref[:, cols]

    def grad(b, j):
        return sa_ref[j, pl.ds(b, TILE, stride=SUB), :]

    rows = row_scales(x_ref, lambda b, j, cols: grad(b, j) * (1.0 + sc_ref[:, cols]))
    back = [rstd * rstd * rstd * mean for rstd, mean in rows]
    for j, cols in lane_tiles():
        scale = 1.0 + sc_ref[:, cols]
        total = gs_ref[:, cols]
        for b in range(SUB):
            xf = x_ref[b, :, cols].astype(F32)
            dn = grad(b, j) * rows[b][0]
            total = total + both(dn * xf)
            gx_ref[b, :, cols] = (gz_ref[b, :, cols].astype(F32) + (dn * scale - xf * back[b])).astype(BF)
        gs_ref[:, cols] = total


def gx_call(dn, x, gz, scale):
    return row_call(gx_kernel, 70, (dn, x, gz, scale), [ROW_BLOCK, SEQ_BLOCK, SEQ_BLOCK, ONE_ROW], [SEQ_BLOCK, SUM_BLOCK],
                    [sds((GRP * SUB, TOK, DM), BF), sds((SUB, DM), F32)], 1)


def cast_kernel(*refs):
    outs, tok = refs[-4:-1], refs[-1]
    tok[...] = jnp.zeros_like(tok)
    for which in range(2):
        @pl.when(pl.program_id(0) == which)
        def _(which=which):
            for kind in range(3):
                outs[kind][...] = refs[3 * which + kind][0].astype(BF)


def cast_call(phase, a_half, b_half, prev, after):
    def half_row(s):
        core = lax.axis_index("cp")
        return core + s * (1 - 2 * core)

    def half_spec(which, kind):
        return pl.BlockSpec((1, HALF, CH), lambda s, r: ((r * s if which else r * (1 - s) + 3 * s), kind, 0))

    in_specs = [half_spec(which, kind) for which in range(2) for kind in range(3)]
    args = [a_half] * 3 + [b_half] * 3
    alias = {}
    if prev is not None:
        alias = {len(args) + k: k for k in range(3)}
        args += list(prev)
        in_specs += [ANY] * 3
    args += list(after)
    in_specs += [ANY] * len(after)
    *weights, tok = pl.pallas_call(
        cast_kernel, grid=(2, 4), in_specs=in_specs,
        out_specs=[pl.BlockSpec((HALF, CH), lambda s, r: (half_row(s), r * 2 + phase % 2))] * 3 + [pl.BlockSpec((SUB, LANES), lambda s, r: (0, 0))],
        out_shape=[sds((DM, HALF), BF)] * 3 + [TOKEN], input_output_aliases=alias,
        compiler_params=params(), cost_estimate=cost(25))(*args)
    return weights, tok


def run(steps):
    for _ in steps:
        pass


LAG_TAPS, LAG_GATES, LAG_GRADS, LAG_BACK, LAG_DX = 4, 5, 10, 11, 15
STRIPS = tuple(range(0, PIECE, STRIP))


def rnn_kernel(own, groups, units, chip_of, col_of, *refs):
    it = iter(refs)

    def take(count):
        return [next(it) for _ in range(count)]

    n_hbm, g_hbm, wy_hbm, wx_hbm, wo_hbm = take(5)
    gate_hbm = take(1 if own else 2)
    par_ref, pos_ref = take(2)
    if own:
        outs = take(9)
        conv_hbm, dpre_hbm, stat_ref = take(3)
    else:
        take(3)
        outs = take(3)
    tok_ref, = take(1)
    nbuf, gbuf, wbuf, wgf, wgb, py, dm, xbuf, ab, uv, yb, w1b, pb, qab, qib, mib, dbuf, conv, pre, dpre, dconv, st_m, st_y, st_x, st1, st2, enter, csend, crecv = take(29)
    if own:
        rb = next(it)
    n_sem, g_sem, w_sem, wg_sem, o_sem, c_send, c_recv, d_send, d_recv, x_send, x_recv = take(11)
    if own:
        p_sem = next(it)

    core = lax.axis_index("cp")
    peer = 1 - core
    pieces = GROWS // PIECE
    steps = units * pieces
    xslots = xbuf.shape[0]
    share = 220 if own else 180

    def unit_of(q):
        return lax.div(q, pieces), lax.rem(q, pieces)

    def block_of(u):
        return lax.div(u, groups), lax.rem(u, groups)

    def al(val, mult=SUB):
        return pl.multiple_of(val, mult)

    def row_copy(q, which):
        u, i = unit_of(q)
        rows = pl.ds(al(block_of(u)[1] * GROWS + i * PIECE, PIECE), PIECE)
        slot = lax.rem(q, 2)
        src, dst, sem = ((n_hbm, nbuf, n_sem), (g_hbm, gbuf, g_sem))[which]
        return pltpu.make_async_copy(src.at[rows], dst.at[slot], sem.at[slot])

    def weight_copy(blk, which):
        slot = lax.rem(blk, 2)
        src = (wy_hbm, wx_hbm, wo_hbm)[which]
        return pltpu.make_async_copy(src.at[:, pl.ds(al(col_of(blk, False) * CH, CH), CH)], wbuf.at[slot, which], w_sem.at[slot, which])

    def gate_copies(blk):
        slot = lax.rem(blk, 2)
        chip, j = chip_of(blk)
        if own:
            return [pltpu.make_async_copy(gate_hbm[0].at[j], wgf.at[slot], wg_sem.at[0, slot])]
        rows = pl.ds(3 * HALF, CH)
        return [pltpu.make_async_copy(gate_hbm[w].at[chip, rows], wgf.at[slot, (peer if w else core)], wg_sem.at[w, slot]) for w in range(2)]

    def out_copy(q, lag, which, forward):
        u, i = unit_of(q - lag)
        blk, grp = block_of(u)
        p = i if forward is None else i + forward * (pieces - 1 - 2 * i)
        slot = lax.rem(q, 2)
        src = (st_m, st_y, st_x)[which % 3].at[slot]
        rows = pl.ds(al(grp * GROWS + p * PIECE, PIECE), PIECE)
        col = blk if which >= 6 else col_of(blk, True)
        return pltpu.make_async_copy(src, outs[which].at[rows, pl.ds(al(col * CH, CH), CH)], o_sem.at[which, slot])

    def conv_copy(q):
        u, i = unit_of(q - LAG_TAPS)
        blk, grp = block_of(u)
        p = i + core * (pieces - 1 - 2 * i)
        slot = lax.rem(q, 2)
        rows = pl.ds(al(grp * GROWS + p * PIECE, PIECE), PIECE)
        return pltpu.make_async_copy(conv.at[slot], conv_hbm.at[rows, pl.ds(al(blk * CH, CH), CH)], p_sem.at[0, slot])

    def dpre_copy(q):
        u, i = unit_of(q - LAG_GRADS)
        blk, grp = block_of(u)
        p = i + peer * (pieces - 1 - 2 * i)
        slot = lax.rem(q, 2)
        rows = pl.ds(al(grp * GROWS + p * PIECE, PIECE), PIECE)
        return pltpu.make_async_copy(dpre.at[slot], dpre_hbm.at[rows, pl.ds(al(blk * 2 * CH, CH), 2 * CH)], p_sem.at[1, slot])

    def remote(src, dst, send, recv):
        return pltpu.make_async_remote_copy(src_ref=src, dst_ref=dst, send_sem=send, recv_sem=recv, device_id={"cp": peer}, device_id_type=pl.DeviceIdType.MESH)

    def halo_copy(u):
        slot, sem = lax.rem(u, xslots), lax.rem(u, 2)
        return remote(xbuf.at[slot, pl.ds(HALO + GROWS - 24, 24)], xbuf.at[slot, pl.ds(HALO - 24, 24)], x_send.at[sem], x_recv.at[sem])

    def carry_copy(u):
        slot = lax.rem(u, 2)
        return remote(csend.at[slot], crecv.at[slot], c_send.at[slot], c_recv.at[slot])

    def dconv_copy(u):
        slot = lax.rem(u, 2)
        return remote(dbuf.at[slot, pl.ds(0, 24)], dbuf.at[slot, pl.ds(GROWS, 24)], d_send.at[slot], d_recv.at[slot])

    def out_copies(q):
        grads = (q >= LAG_GRADS) & (q < steps + LAG_GRADS)
        last = (q >= LAG_DX) & (q < steps + LAG_DX)
        made = []
        for which in range(len(outs)):
            lag, forward, when = (LAG_DX, None, last) if which % 3 == 2 else (LAG_GRADS, peer, grads)
            if own and which < 6:
                late = q - lag >= steps // 2
                when = when & (late if which >= 3 else ~late)
            made.append((when, functools.partial(out_copy, q, lag, which, forward)))
        if own:
            made += [((q >= LAG_TAPS) & (q < steps + LAG_TAPS), lambda: conv_copy(q)), (grads, lambda: dpre_copy(q))]
        return made

    def at(q, lag, i):
        return (q >= lag) & (q < steps + lag) & (lax.rem(q - lag + pieces, pieces) == i)

    def rowpos(base, k):
        pos = pos_ref[pl.ds(al(base + k * SUB), STRIP), :]
        return jnp.concatenate([pos, pos], axis=1)

    def param(blk, k):
        chip, j = chip_of(blk)
        return par_ref[chip, j, k:k + 1, :]

    def stage_at(q, lag):
        u, i = unit_of(jnp.maximum(q - lag, 0))
        blk, grp = block_of(u)
        return u, i, blk, grp

    zero = lax.div(core, 2)

    def folded(val):
        return jnp.sum(val.reshape(STRIP // SUB, SUB, CH), axis=0)

    def scan_piece(slot, p, back, state):
        first = (p * (PIECE // SUB) + back * (PIECE // SUB - 1)) * SUB
        ahead, stride = first + SUB * back, SUB - 16 * back
        for tt in range(PIECE // SUB):
            decay = ab[slot, pl.ds(al(ahead + tt * stride), SUB), :]
            at_t = pl.ds(al(first + tt * stride + SUB), SUB)
            state = uv[back, slot, at_t, :] + decay * state
            uv[back, slot, at_t, :] = state
            yield 6
        return state

    def products(q):
        u, i, blk, _ = stage_at(q, 0)
        slot, w, us, xs = lax.rem(q, 2), lax.rem(blk, 2), lax.rem(u, 2), lax.rem(u, xslots)
        totals = []
        for src, kind in ((nbuf, 1), (nbuf, 0), (gbuf, 2)):
            total = None
            for k in range(0, DM, KSTEP):
                part = jnp.dot(src[slot, :, k:k + KSTEP], wbuf[w, kind, k:k + KSTEP], preferred_element_type=F32)
                total = part if total is None else total + part
                yield
            if kind == 1:
                total = (total + param(blk, 11)).astype(BF).astype(F32)
                xbuf[xs, pl.ds(al(i * PIECE + HALO), PIECE), :] = total
            totals.append(total)
        yield
        rows = pl.ds(al(i * PIECE, PIECE), PIECE)
        py[us, rows, :] = totals[1] + param(blk, 10)
        dm[us, rows, :] = totals[2]

    def taps(q):
        u, i, blk, grp = stage_at(q, LAG_TAPS)
        base = (i + core * (pieces - 1 - 2 * i)) * PIECE
        xs, cs = lax.rem(u, xslots), lax.rem(q, 2)
        par = [param(blk, k) for k in range(5)]
        for rt in STRIPS:
            pos = rowpos(grp * POS_ROWS + base + rt, 0)
            acc = par[0]
            for k in range(4):
                xk = xbuf[xs, pl.ds(al(base + rt + HALO - SUB * k), STRIP), :]
                if k:
                    xk = jnp.where(pos >= float(k), xk, 0.0)
                acc = acc + xk * par[1 + k]
            conv[cs, rt:rt + STRIP, :] = acc.astype(BF)
            yield 34
        pre[:PIECE] = jnp.dot(conv[cs], wgb[lax.rem(blk, 2)], preferred_element_type=F32)

    def gates(q):
        u, i, blk, grp = stage_at(q, LAG_GATES)
        p = i + core * (pieces - 1 - 2 * i)
        slot, cs = lax.rem(u, 2), lax.rem(q + 1, 2)
        base = p * PIECE
        ba, bi, kh = (param(blk, k) for k in range(5, SUB))
        for rt in STRIPS:
            rd = pl.ds(al(rt + zero * STRIP, STRIP), STRIP)
            rows = pl.ds(al(base + rt, STRIP), STRIP)
            rows8 = pl.ds(al(base + rt + SUB), STRIP)
            v = py[slot, rows, :]
            dmv = dm[slot, rows, :]
            v2 = v * v
            g = 0.5 * jnp.tanh(v * (v2 * GELU_K1 + GELU_K0)) + 0.5
            y = v * g
            yb[slot, rows, :] = y
            w1b[slot, rows, :] = dmv * (g + (v * (g - g * g)) * (v2 * (6.0 * GELU_K1) + 2.0 * GELU_K0))
            uv[1, slot, rows8, :] = dmv * y
            r2 = jnp.tanh(pre[rd, :CH] + ba) + 1.0
            thi = jnp.tanh(pre[rd, CH:] + bi)
            rate = jnp.where(rowpos(grp * POS_ROWS + base + rt, 0) < 0.5, FAR, r2 * kh)
            a = jnp.exp2(rate * -LOG2E)
            msq = jnp.tanh(rate) * (1.0 + a * a)
            rs = lax.rsqrt(jnp.maximum(msq, TINY))
            c = conv[cs, rt:rt + STRIP, :].astype(F32)
            gi = 0.5 * thi + 0.5
            mi = (msq * rs) * gi
            u_in = mi * c
            ab[slot, rows, :] = a
            mib[slot, rows, :] = mi
            uv[0, slot, rows8, :] = u_in
            pb[slot, rows, :] = (gi * c) * (a * rs)
            qab[slot, rows, :] = (a * rate) * (2.0 - r2)
            qib[slot, rows, :] = u_in * (1.0 - thi)
            if own:
                rb[slot, rows, :] = a * r2
            yield 112
        state = yield from scan_piece(slot, p, core, jnp.where(i == 0, 0.0, st1[...]))
        st1[...] = state
        csend[slot] = ab[slot, pl.ds(al(peer * GROWS), SUB), :] * state

    def grads(q):
        _, i, blk, _ = stage_at(q, LAG_GRADS)
        p = i + peer * (pieces - 1 - 2 * i)
        slot = lax.rem(lax.div(q + 3 * pieces - LAG_GRADS, pieces) + 1, 2)
        so = lax.rem(q, 2)
        base = p * PIECE
        entering = enter[...]
        uv[0, slot, pl.ds(0, SUB), :] = jnp.where(core == 1, entering, 0.0)
        st2[...] = yield from scan_piece(slot, p, peer, jnp.where(i == 0, entering, st2[...]))
        sums = [jnp.zeros((SUB, CH), F32)] * 4
        for rt in STRIPS:
            rl = slice(rt, rt + STRIP)
            rows = pl.ds(al(base + rt, STRIP), STRIP)
            rows8 = pl.ds(al(base + rt + SUB), STRIP)
            hid = uv[0, slot, rows8, :]
            dh = uv[1, slot, rows8, :]
            st_m[so, rl, :] = (hid * yb[slot, rows, :]).astype(BF)
            dpy = w1b[slot, rows, :] * hid
            st_y[so, rl, :] = dpy.astype(BF)
            g1 = dh * (pb[slot, rows, :] - uv[0, slot, rows, :])
            dpa = g1 * qab[slot, rows, :]
            dpi = dh * qib[slot, rows, :]
            dconv[rl, :] = dh * mib[slot, rows, :]
            dpre[so, rl, :CH] = dpa.astype(BF)
            dpre[so, rl, CH:] = dpi.astype(BF)
            if own:
                for k, val in enumerate((dpy, dpa, dpi, g1 * rb[slot, rows, :])):
                    sums[k] = sums[k] + folded(val)
            yield 56
        if own:
            for k in range(4):
                stat_ref[blk, k * SUB:k * SUB + SUB, :] += jnp.where(q >= LAG_GRADS, sums[k], 0.0)

    def back(q):
        u, i, blk, grp = stage_at(q, LAG_BACK)
        base = (i + peer * (pieces - 1 - 2 * i)) * PIECE
        slot, so = lax.rem(u, 2), lax.rem(q + 1, 2)
        xs = lax.rem(lax.div(jnp.maximum(q, LAG_BACK - pieces) - LAG_BACK + 4 * pieces, pieces), xslots)
        val = lax.dot_general(dpre[so], wgb[lax.rem(blk, 2)], NT, preferred_element_type=F32)
        dbuf[slot, pl.ds(al(base, PIECE), PIECE), :] = dconv[...] + val
        yield 60
        if own:
            sums = [jnp.zeros((SUB, CH), F32)] * 5
            for rt in STRIPS:
                pos = rowpos(grp * POS_ROWS + base + rt, 0)
                dc = dbuf[slot, pl.ds(al(base + rt, STRIP), STRIP), :]
                sums[0] = sums[0] + folded(dc)
                for k in range(4):
                    xk = xbuf[xs, pl.ds(al(base + rt + HALO - SUB * k), STRIP), :]
                    if k:
                        xk = jnp.where(pos >= float(k), xk, 0.0)
                    sums[1 + k] = sums[1 + k] + folded(dc * xk)
                yield 40
            for k in range(5):
                stat_ref[blk, (5 + k) * SUB:(5 + k) * SUB + SUB, :] += jnp.where(q >= LAG_BACK, sums[k], 0.0)

    def taps_back(q):
        u, i, blk, grp = stage_at(q, LAG_DX)
        slot, so = lax.rem(u, 2), lax.rem(q, 2)
        base = i * PIECE
        par = [param(blk, k) for k in range(1, 5)]
        total = jnp.zeros((SUB, CH), F32)
        for rt in STRIPS:
            acc = dbuf[slot, pl.ds(al(base + rt), STRIP), :] * par[0]
            for k in range(1, 4):
                dk = dbuf[slot, pl.ds(al(base + rt + SUB * k), STRIP), :]
                acc = acc + jnp.where(rowpos(grp * POS_ROWS + base + rt, k) >= float(k), dk, 0.0) * par[k]
            st_x[so, rt:rt + STRIP, :] = acc.astype(BF)
            if own:
                total = total + folded(acc)
            yield 32
        if own:
            stat_ref[blk, 32:40, :] += jnp.where(q >= LAG_DX, total, 0.0)

    def start_of_step(q):
        for when, make in out_copies(q - 2):
            @pl.when(when)
            def _(make=make):
                make().wait()

        @pl.when(at(q, LAG_TAPS, 3) & (core == 0))
        def _():
            halo_copy(lax.div(q - LAG_TAPS, pieces)).wait_send()

        @pl.when(at(q, LAG_TAPS, 3) & (core == 1))
        def _():
            halo_copy(lax.div(q - LAG_TAPS, pieces)).wait_recv()

        @pl.when(at(q, LAG_GRADS, 0))
        def _():
            u = lax.div(q - LAG_GRADS, pieces)
            carry_copy(u).wait()
            enter[...] = crecv[lax.rem(u, 2)]

        @pl.when(at(q, LAG_DX, 3))
        def _():
            dconv_copy(lax.div(q - LAG_DX, pieces)).wait()

        @pl.when((q >= LAG_TAPS) & (q < steps + LAG_TAPS) & (lax.rem(q - LAG_TAPS + groups * pieces, groups * pieces) == 0))
        def _():
            blk = lax.div(q - LAG_TAPS, groups * pieces)
            for cp in gate_copies(blk):
                cp.wait()
            slot = lax.rem(blk, 2)
            wgb[slot, :, :CH] = wgf[slot, 0].astype(BF)
            wgb[slot, :, CH:] = wgf[slot, 1].astype(BF)

            @pl.when(blk + 1 < units // groups)
            def _():
                for cp in gate_copies(blk + 1):
                    cp.start()

    def end_of_step(q):
        for when, make in out_copies(q):
            @pl.when(when)
            def _(make=make):
                make().start()

        @pl.when(at(q, LAG_TAPS, 0) & (core == 0))
        def _():
            halo_copy(lax.div(q - LAG_TAPS, pieces)).start()

        @pl.when(at(q, LAG_GATES, 3))
        def _():
            carry_copy(lax.div(q - LAG_GATES, pieces)).start()

        @pl.when(at(q, LAG_BACK, 3))
        def _():
            dconv_copy(lax.div(q - LAG_BACK, pieces)).start()

    for which in range(2):
        row_copy(0, which).start()
    for which in range(3):
        weight_copy(0, which).start()
    for cp in gate_copies(0):
        cp.start()
    tok_ref[...] = jnp.zeros_like(tok_ref)
    for slot in range(2):
        ab[slot, pl.ds(GROWS, SUB), :] = jnp.ones((SUB, CH), F32)
    if own:
        stat_ref[...] = jnp.zeros_like(stat_ref)
    barrier = pltpu.get_barrier_semaphore()
    pl.semaphore_signal(barrier, inc=1, device_id={"cp": peer}, device_id_type=pl.DeviceIdType.MESH)
    pl.semaphore_wait(barrier, 1)

    def full_step(q, _):
        for which in range(2):
            row_copy(q, which).wait()

        @pl.when(q + 1 < steps)
        def _():
            for which in range(2):
                row_copy(q + 1, which).start()

        @pl.when(lax.rem(q, groups * pieces) == 0)
        def _():
            blk = lax.div(q, groups * pieces)
            for which in range(3):
                weight_copy(blk, which).wait()

            @pl.when(blk + 1 < units // groups)
            def _():
                for which in range(3):
                    weight_copy(blk + 1, which).start()

        start_of_step(q)
        product_steps, spent, made = products(q), share, 0
        for stage in (taps_back, back, grads, gates, taps):
            for bundles in stage(q):
                spent += bundles
                while spent >= share and made < 3 * DM // KSTEP:
                    spent -= share
                    made += 1
                    next(product_steps)
        run(product_steps)
        end_of_step(q)
        return 0

    lax.fori_loop(0, steps, full_step, 0)

    def drain_step(q, _):
        start_of_step(q)
        for lag, stage in ((LAG_DX, taps_back), (LAG_BACK, back), (LAG_GRADS, grads), (LAG_GATES, gates), (LAG_TAPS, taps)):
            @pl.when(q < steps + lag)
            def _(stage=stage):
                run(stage(q))
        end_of_step(q)
        return 0

    lax.fori_loop(steps, steps + LAG_DX, drain_step, 0)
    for q in (steps + LAG_DX, steps + LAG_DX + 1):
        for when, make in out_copies(jnp.int32(q - 2)):
            @pl.when(when)
            def _(make=make):
                make().wait()


def rnn_call(phase, groups, n, gz, weights, gate_src, par, pos, acts):
    own = phase is None
    units = (4 if own else 3) * groups

    def chip_of(blk):
        return (0, blk) if own else (lax.rem(lax.axis_index("tp") + 1 + blk, 4), 0)

    def col_of(blk, merged):
        if own:
            return lax.axis_index("tp") * 2 + lax.rem(blk, 2) if merged else blk
        return chip_of(blk)[0] * 2 + phase % 2

    args = [n, gz, *weights, *gate_src, par, pos, *acts]
    in_specs = [ANY] * (5 + len(gate_src)) + [VM] * 2 + [ANY] * len(acts)
    out_specs = [ANY] * 3
    out_shape = [sds((ROWS, HALF), BF)] * 3
    alias = {9 + k: k for k in range(len(acts))}
    if own:
        out_specs = [ANY] * 11 + [VM]
        out_shape = out_shape * 2 + [sds((ROWS, 4 * CH), BF)] * 4 + [sds((ROWS, SUB * CH), BF), sds((4, 80, CH), F32)]
    out_specs = out_specs + [VM]
    out_shape = out_shape + [TOKEN]

    def buf(slots, rows, dtype=F32, cols=CH):
        return pltpu.VMEM((slots, rows, cols), dtype)

    piece32 = pltpu.VMEM((PIECE, CH), F32)
    scratch = [buf(2, PIECE, BF, DM), buf(2, PIECE, BF, DM), pltpu.VMEM((2, 3, DM, CH), BF), pltpu.VMEM((2, 2, CH, CH), F32), buf(2, CH, BF, 2 * CH),
               buf(2, GROWS), buf(2, GROWS), buf(4 if own else 2, GROWS + HALO), buf(2, GROWS + SUB),
               pltpu.VMEM((2, 2, GROWS + SUB, CH), F32)] + [buf(2, GROWS)] * 6 + [buf(2, GROWS + HALO), buf(2, PIECE, BF),
               pltpu.VMEM((PIECE + STRIP, 2 * CH), F32), buf(2, PIECE, BF, 2 * CH), piece32] + [buf(2, PIECE, BF)] * 3 + [pltpu.VMEM((SUB, CH), F32)] * 3 + [buf(2, SUB)] * 2
    dma = pltpu.SemaphoreType.DMA
    sems = [dma((2,)), dma((2,)), dma((2, 3)), dma((2, 2)), dma((9 if own else 3, 2))] + [dma((2,))] * 6
    if own:
        scratch.append(buf(2, GROWS))
        sems.append(dma((2, 2)))
    return pl.pallas_call(
        functools.partial(rnn_kernel, own, groups, units, chip_of, col_of), in_specs=in_specs, out_specs=out_specs, out_shape=out_shape,
        scratch_shapes=scratch + sems, input_output_aliases=alias,
        compiler_params=params(collective_id=0 if own else 1 + phase, has_side_effects=True),
        cost_estimate=cost(10 * units))(*args)


def layer(x_in, grad_z, seg_pos, norm_scale, w_x, b_x, w_y, b_y, conv_w, conv_b, w_a, b_a, w_i, b_i, a_param, w_out, b_out):
    core = lax.axis_index("cp")
    swap = [(0, 1), (1, 0)]
    half = core * HALF

    zero = jnp.zeros_like(a_param)
    rows = [conv_b.astype(F32)] + [conv_w[k].astype(F32) for k in range(4)] + [0.5 * b_a.astype(F32), 0.5 * b_i.astype(F32), 4.0 * jax.nn.softplus(a_param), zero, zero,
            b_y.astype(F32), b_x.astype(F32)] + [zero] * 4
    par_own = jnp.stack(rows).reshape(16, 4, CH).transpose(1, 0, 2)
    wg_own = jnp.stack([w_a, w_i], axis=1).astype(F32) * 0.5
    wg_mine = lax.dynamic_index_in_dim(wg_own, core, 1, keepdims=False)

    got = []
    for j in range(4):
        cols = j * CH
        parts = [lax.dynamic_slice(w_y, (half, cols), (HALF, CH)).astype(F32), lax.dynamic_slice(w_x, (half, cols), (HALF, CH)).astype(F32),
                 lax.dynamic_slice(w_out, (cols, half), (CH, HALF)).T.astype(F32), wg_mine[j], par_own[j]]
        mine = lax.optimization_barrier(jnp.concatenate(parts, axis=0))
        got.append(lax.all_gather(mine, "tp"))

    def partner(val):
        return lax.ppermute(val, "cp", swap)

    pos = seg_pos.astype(jnp.int32)
    later = jnp.where(core == 0, partner(pos[:, :SUB]), -1)
    pos = jnp.concatenate([pos, later], axis=1).reshape(GRP, SUB, TOK + SUB).transpose(0, 2, 1).astype(F32)
    pos = jnp.broadcast_to(pos.reshape(GRP * POS_ROWS, 1), (GRP * POS_ROWS, LANES))

    scale = norm_scale.astype(F32)[None]
    n, gz, gb = norm_call(x_in, grad_z, scale)

    first = rnn_call(None, GRP, n, gz, (w_y, w_x, w_out.T), (wg_own,), par_own[None], pos, ())
    sets, (omixed, ody, odx, conv16, dpre16, stats) = [first[:3], first[3:6]], first[6:12]
    weights = [None, None]

    def dot(lhs, rhs, dims):
        return lax.dot_general(lhs, rhs, dims, preferred_element_type=F32)

    def phase(j, deps):
        s = j // 2
        other = partner(got[j])
        weights[s], _ = cast_call(j, got[j], other, weights[s], deps)
        par = got[j][:, None, 3 * HALF + CH:]
        *acts, token = rnn_call(j, GRP, n, gz, weights[s], (got[j], other), par, pos, sets[s])
        sets[s] = acts
        return token

    g_w_x = dot(n, odx, TN)
    g_w_y = dot(n, ody, TN)
    phase(0, (g_w_x, g_w_y))
    g_w_out = dot(omixed, gz, TN)
    g_gate = 0.5 * jnp.einsum("rhk,rhj->hkj", conv16.reshape(ROWS, 4, CH), dpre16.reshape(ROWS, 4, 2 * CH), preferred_element_type=F32)
    stats = jnp.sum(stats.reshape(4, 10, SUB, CH), axis=2).transpose(1, 0, 2).reshape(10, 4 * CH)
    phase(1, (g_w_out, g_gate))
    g_w_x, g_w_y, g_w_out, g_gate = lax.psum((g_w_x, g_w_y, g_w_out, g_gate), "cp")
    z_acc = dot(sets[0][0], weights[0][2], NT)
    dn = dot(sets[0][1], weights[0][0], NT)
    dn = dot(sets[0][2], weights[0][1], NT) + dn
    phase(2, (z_acc, dn))
    phase(3, ())
    z_acc = dot(sets[1][0], weights[1][2], NT) + z_acc
    z_out = z_call(z_acc, x_in, b_out.astype(F32)[None])
    dn = dot(sets[1][1], weights[1][0], NT) + dn
    dn = dot(sets[1][2], weights[1][1], NT) + dn
    grad_x, gs = gx_call(dn, x_in, grad_z, scale)

    g_scale, stats, g_b_out = lax.psum((jnp.sum(gs, axis=0), stats, jnp.sum(gb, axis=0)), "cp")
    return (z_out, grad_x, g_scale, g_w_x, stats[4], g_w_y, stats[0], stats[6:10], stats[5], g_gate[:, :, :CH], 0.5 * stats[1],
            g_gate[:, :, CH:], 0.5 * stats[2], 4.0 * jax.nn.sigmoid(a_param) * stats[3], g_w_out, g_b_out)


def solution(mesh):
    return jax.shard_map(layer, mesh=mesh, in_specs=IN_SPECS, out_specs=OUT_SPECS, check_vma=False)
```

```python
import functools
import jax
import jax.numpy as jnp
from jax import lax
from jax.experimental import pallas as pl
from jax.experimental.pallas import tpu as pltpu
from jax.sharding import PartitionSpec as P

NORM_EPS = 1e-6
TINY, FAR = 1e-37, 1e4
LOG2E = 1.4426950408889634
GELU_K0 = 0.7978845608028654
GELU_K1 = GELU_K0 * 0.044715
SUB = 8
TOK, GRP, CH, DM, LANES, TILE = 128, 4, 256, 4096, 128, 16
GROWS = TOK * SUB
ROWS = GRP * GROWS
HALF = DM // 2
PIECE, HALO, WROWS, DEPTH = 256, 32, 1024, 4
KSTEP, STRIP = 1024, 32
POS_ROWS = GROWS + 64
COLS = DM // LANES
BF, F32 = jnp.bfloat16, jnp.float32
ANY = pl.BlockSpec(memory_space=pl.ANY)
VM = pl.BlockSpec(memory_space=pltpu.VMEM)
VMEM_MOST = 67000000
NT = (((1,), (1,)), ((), ()))
TN = (((0,), (0,)), ((), ()))
SEQ, ALL, CHAN, COL, BLK, ROW = P(None, "cp", None), P(), P("tp"), P(None, "tp"), P("tp", None, None), P("tp", None)
PARAMS = (COL, CHAN, COL, CHAN, COL, CHAN, BLK, CHAN, BLK, CHAN, CHAN, ROW, ALL)
IN_SPECS = (SEQ, SEQ, P(None, "cp"), ALL) + PARAMS
OUT_SPECS = (SEQ, SEQ, ALL) + PARAMS


def sds(shape, dtype):
    return jax.ShapeDtypeStruct(shape, dtype)


def cost(us):
    return pl.CostEstimate(flops=int(us * 1e9), bytes_accessed=int(us * 1e6), transcendentals=0)


def params(**kw):
    return pltpu.CompilerParams(vmem_limit_bytes=VMEM_MOST, **kw)


def lane_tiles():
    return [(j, slice(j * LANES, (j + 1) * LANES)) for j in range(COLS)]


NTOK = TOK // TILE
FULL_DN, FULL_Z = 20 * SUB * TILE, 24 * SUB * TILE
NBLK = GRP * NTOK
ONE_ROW = pl.BlockSpec((1, DM), lambda i: (0, 0))
SUM_BLOCK = pl.BlockSpec((SUB, DM), lambda i: (0, 0))
TURN = pltpu.VMEM((COLS, SUB * TILE, LANES), F32)


def seq_block(first):
    return pl.BlockSpec((SUB, TILE, DM), lambda i: ((first + i) // NTOK, (first + i) % NTOK, 0))


def row_call(kernel, us, blocks, inputs, in_specs, out_specs, out_shape, turns, whole=None):
    first, last = blocks
    alias = {}
    if whole is not None:
        alias = {len(inputs): 0}
        inputs = (*inputs, whole)
        in_specs = in_specs + [ANY]
    return pl.pallas_call(kernel, grid=(last - first,), in_specs=in_specs, out_specs=out_specs, out_shape=out_shape, scratch_shapes=[TURN] * turns,
                          input_output_aliases=alias, compiler_params=params(), cost_estimate=cost(us))(*inputs)


def first_step():
    return pl.program_id(0) == 0


def both(val):
    return val[:SUB] + val[SUB:]


def row_scales(x_ref, more=None):
    found = []
    for b in range(SUB):
        square = other = jnp.zeros((TILE, LANES), F32)
        for j, cols in lane_tiles():
            xf = x_ref[b, :, cols].astype(F32)
            square = square + xf * xf
            if more is not None:
                other = other + xf * more(b, j, cols)
        rstd = lax.rsqrt(jnp.sum(square, axis=-1, keepdims=True) * (1.0 / DM) + NORM_EPS)
        found.append((rstd, jnp.sum(other, axis=-1, keepdims=True) * (1.0 / DM)))
    return found


def norm_kernel(x_ref, gz_ref, sc_ref, n_ref, g_ref, gb_ref, sn_ref, sg_ref):
    @pl.when(first_step())
    def _():
        gb_ref[...] = jnp.zeros_like(gb_ref)

    rows = row_scales(x_ref)
    for j, cols in lane_tiles():
        scale = 1.0 + sc_ref[:, cols]
        total = gb_ref[:, cols]
        for b in range(SUB):
            gf = gz_ref[b, :, cols].astype(F32)
            total = total + both(gf)
            sn_ref[j, pl.ds(b, TILE, stride=SUB), :] = x_ref[b, :, cols].astype(F32) * rows[b][0] * scale
            sg_ref[j, pl.ds(b, TILE, stride=SUB), :] = gf
        gb_ref[:, cols] = total
        n_ref[:, cols] = sn_ref[j].astype(BF)
        g_ref[:, cols] = sg_ref[j].astype(BF)


ROW_BLOCK = pl.BlockSpec((SUB * TILE, DM), lambda i: (i, 0))


def norm_call(x, gz, scale):
    seq = seq_block(0)
    return row_call(norm_kernel, 60, (0, NBLK), (x, gz, scale), [seq, seq, ONE_ROW], [ROW_BLOCK, ROW_BLOCK, SUM_BLOCK],
                    [sds((ROWS, DM), BF), sds((ROWS, DM), BF), sds((SUB, DM), F32)], 2)


def z_kernel(acc_ref, x_ref, bo_ref, *refs):
    z_ref, sa_ref = refs[-2:]
    for j, cols in lane_tiles():
        sa_ref[j] = acc_ref[:, cols]
    for b in range(SUB):
        for j, cols in lane_tiles():
            z_ref[b, :, cols] = (x_ref[b, :, cols].astype(F32) + (sa_ref[j, pl.ds(b, TILE, stride=SUB), :] + bo_ref[:, cols])).astype(BF)


def z_call(blocks, acc, x, b_out, whole=None):
    seq = seq_block(blocks[0])
    return row_call(z_kernel, 40, blocks, (acc, x, b_out), [ROW_BLOCK, seq, ONE_ROW], seq, sds((GRP * SUB, TOK, DM), BF), 1, whole)


def gx_kernel(dn_ref, x_ref, gz_ref, sc_ref, *refs):
    gx_ref, gs_ref, sa_ref = refs[-3:]

    @pl.when(first_step())
    def _():
        gs_ref[...] = jnp.zeros_like(gs_ref)

    for j, cols in lane_tiles():
        sa_ref[j] = dn_ref[:, cols]

    def grad(b, j):
        return sa_ref[j, pl.ds(b, TILE, stride=SUB), :]

    rows = row_scales(x_ref, lambda b, j, cols: grad(b, j) * (1.0 + sc_ref[:, cols]))
    back = [rstd * rstd * rstd * mean for rstd, mean in rows]
    for j, cols in lane_tiles():
        scale = 1.0 + sc_ref[:, cols]
        total = gs_ref[:, cols]
        for b in range(SUB):
            xf = x_ref[b, :, cols].astype(F32)
            dn = grad(b, j) * rows[b][0]
            total = total + both(dn * xf)
            gx_ref[b, :, cols] = (gz_ref[b, :, cols].astype(F32) + (dn * scale - xf * back[b])).astype(BF)
        gs_ref[:, cols] = total


def gx_call(blocks, dn, x, gz, scale, whole=None):
    seq = seq_block(blocks[0])
    return row_call(gx_kernel, 50, blocks, (dn, x, gz, scale), [ROW_BLOCK, seq, seq, ONE_ROW], [seq, SUM_BLOCK],
                    [sds((GRP * SUB, TOK, DM), BF), sds((SUB, DM), F32)], 1, whole)


def run(steps):
    for _ in steps:
        pass


LAG_TAPS, LAG_GATES, LAG_GRADS, LAG_BACK, LAG_DX = 4, 5, 10, 11, 15
STRIPS = tuple(range(0, PIECE, STRIP))


def rnn_kernel(own, groups, units, chip_of, col_of, *refs):
    it = iter(refs)

    def take(count):
        return [next(it) for _ in range(count)]

    n_hbm, g_hbm = take(2)
    if own:
        own_w = take(3)
        gate_hbm = take(1)
    else:
        gate_hbm = take(2)
    par_ref, pos_ref = take(2)
    if not own:
        take(4)
    mixed_hbm, dyx_hbm, wyx_hbm, wz_hbm = take(4)
    outs = [mixed_hbm, dyx_hbm, dyx_hbm]
    if own:
        outs += take(3)
        conv_hbm, dpre_hbm, stat_ref = take(3)
    nbuf, gbuf, wbuf, wgf, wgb, py, dm, xbuf, ab, uv, yb, w1b, pb, qab, qib, mib, dbuf, conv, pre, dpre, dconv, st_m, st_y, st_x, st1, st2, enter, csend, crecv = take(29)
    if own:
        rb = next(it)
    if not own:
        stage = next(it)
    n_sem, g_sem, w_sem, wo_sem, wg_sem, o_sem, c_send, c_recv, d_send, d_recv, x_send, x_recv = take(12)
    if own:
        p_sem = next(it)

    core = lax.axis_index("cp")
    peer = 1 - core
    pieces = GROWS // PIECE
    steps = units * pieces
    xslots = xbuf.shape[0]
    share = 220 if own else 180

    def unit_of(q):
        return lax.div(q, pieces), lax.rem(q, pieces)

    def block_of(u):
        return lax.div(u, groups), lax.rem(u, groups)

    def al(val, mult=SUB):
        return pl.multiple_of(val, mult)

    def row_copy(q, which):
        u, i = unit_of(q)
        rows = pl.ds(al(block_of(u)[1] * GROWS + i * PIECE, PIECE), PIECE)
        slot = lax.rem(q, 2)
        src, dst, sem = ((n_hbm, nbuf, n_sem), (g_hbm, gbuf, g_sem))[which]
        return pltpu.make_async_copy(src.at[rows], dst.at[slot], sem.at[slot])

    blocks, turns = units // groups, groups * pieces

    def weight_in(blk, kind):
        slot = lax.rem(blk, 2)
        return pltpu.make_async_copy(own_w[kind].at[:, pl.ds(al(blk * CH, CH), CH)], wbuf.at[slot, kind], w_sem.at[slot, kind])

    def weight_out(blk, kind):
        slot = lax.rem(blk, 2)
        col = col_of(blk, True) * CH + (DM if kind == 1 else 0)
        dst = wz_hbm if kind == 2 else wyx_hbm
        return pltpu.make_async_copy(wbuf.at[slot, kind], dst.at[:, pl.ds(al(col, CH), CH)], wo_sem.at[slot, kind])

    per_half = 3 * HALF // WROWS

    def strip_slot(t, half):
        return lax.rem(t + half * per_half, DEPTH)

    def strip_in(blk, t, half):
        rows = pl.ds(al(t * WROWS, WROWS), WROWS)
        return pltpu.make_async_copy(gate_hbm[half].at[chip_of(blk)[0], rows], stage.at[strip_slot(t, half)], w_sem.at[strip_slot(t, half)])

    def strip_cast(blk, t, half):
        per_kind = HALF // WROWS
        row = (peer if half else core) * HALF + lax.rem(t, per_kind) * WROWS
        wbuf[lax.rem(blk, 2), lax.div(t, per_kind), pl.ds(al(row, WROWS), WROWS), :] = stage[strip_slot(t, half)].astype(BF)

    def weight_turn(q):
        blk, t = lax.div(q, turns), lax.rem(q, turns)

        @pl.when((t == 0) & (blk >= 1) & (blk + 1 < blocks))
        def _():
            for kind in range(3):
                weight_out(blk - 1, kind).wait()

        if own:
            @pl.when(t == 0)
            def _():
                for kind in range(3):
                    weight_in(blk, kind).wait()
                    weight_out(blk, kind).start()

                @pl.when(blk + 1 < blocks)
                def _():
                    for kind in range(3):
                        weight_in(blk + 1, kind).start()

            return
        more = blk + 1 < blocks
        for half in range(2):
            done = t - 1 - half * per_half

            @pl.when(more & (done >= 0) & (done < per_half))
            def _(half=half, done=done):
                strip_in(blk + 1, done, half).wait()
                strip_cast(blk + 1, done, half)
        for half in range(2):
            new = t - half * per_half

            @pl.when(more & (new >= 0) & (new < per_half))
            def _(half=half, new=new):
                strip_in(blk + 1, new, half).start()

        @pl.when(more & (t == 2 * per_half + 1))
        def _():
            for kind in range(3):
                weight_out(blk + 1, kind).start()

    def weights_first():
        if own:
            for kind in range(3):
                weight_in(0, kind).start()
            return
        ahead = DEPTH - 1
        for t in range(ahead):
            strip_in(0, t, 0).start()
        for half in range(2):
            def turn(t, _, half=half):
                @pl.when(t + ahead < per_half)
                def _():
                    strip_in(0, t + ahead, half).start()

                if half == 0:
                    @pl.when(t + ahead >= per_half)
                    def _():
                        strip_in(0, t + ahead - per_half, 1).start()
                strip_in(0, t, half).wait()
                strip_cast(0, t, half)
                return 0

            lax.fori_loop(0, per_half, turn, 0)
        for kind in range(3):
            weight_out(0, kind).start()

    def gate_copies(blk):
        slot = lax.rem(blk, 2)
        chip, j = chip_of(blk)
        if own:
            return [pltpu.make_async_copy(gate_hbm[0].at[j], wgf.at[slot], wg_sem.at[0, slot])]
        rows = pl.ds(3 * HALF, CH)
        return [pltpu.make_async_copy(gate_hbm[w].at[chip, rows], wgf.at[slot, (peer if w else core)], wg_sem.at[w, slot]) for w in range(2)]

    def out_copy(q, lag, which, forward):
        u, i = unit_of(q - lag)
        blk, grp = block_of(u)
        p = i if forward is None else i + forward * (pieces - 1 - 2 * i)
        slot = lax.rem(q, 2)
        src = (st_m, st_y, st_x)[which % 3].at[slot]
        rows = pl.ds(al(grp * GROWS + p * PIECE, PIECE), PIECE)
        col = blk if which >= 3 else col_of(blk, True) + (DM // CH if which == 2 else 0)
        return pltpu.make_async_copy(src, outs[which].at[rows, pl.ds(al(col * CH, CH), CH)], o_sem.at[which, slot])

    def conv_copy(q):
        u, i = unit_of(q - LAG_TAPS)
        blk, grp = block_of(u)
        p = i + core * (pieces - 1 - 2 * i)
        slot = lax.rem(q, 2)
        rows = pl.ds(al(grp * GROWS + p * PIECE, PIECE), PIECE)
        return pltpu.make_async_copy(conv.at[slot], conv_hbm.at[blk, rows], p_sem.at[0, slot])

    def dpre_copy(q):
        u, i = unit_of(q - LAG_GRADS)
        blk, grp = block_of(u)
        p = i + peer * (pieces - 1 - 2 * i)
        slot = lax.rem(q, 2)
        rows = pl.ds(al(grp * GROWS + p * PIECE, PIECE), PIECE)
        return pltpu.make_async_copy(dpre.at[slot], dpre_hbm.at[blk, rows], p_sem.at[1, slot])

    def remote(src, dst, send, recv):
        return pltpu.make_async_remote_copy(src_ref=src, dst_ref=dst, send_sem=send, recv_sem=recv, device_id={"cp": peer}, device_id_type=pl.DeviceIdType.MESH)

    def halo_copy(u):
        slot, sem = lax.rem(u, xslots), lax.rem(u, 2)
        return remote(xbuf.at[slot, pl.ds(HALO + GROWS - 24, 24)], xbuf.at[slot, pl.ds(HALO - 24, 24)], x_send.at[sem], x_recv.at[sem])

    def carry_copy(u):
        slot = lax.rem(u, 2)
        return remote(csend.at[slot], crecv.at[slot], c_send.at[slot], c_recv.at[slot])

    def dconv_copy(u):
        slot = lax.rem(u, 2)
        return remote(dbuf.at[slot, pl.ds(0, 24)], dbuf.at[slot, pl.ds(GROWS, 24)], d_send.at[slot], d_recv.at[slot])

    def out_copies(q):
        grads = (q >= LAG_GRADS) & (q < steps + LAG_GRADS)
        last = (q >= LAG_DX) & (q < steps + LAG_DX)
        made = []
        for which in range(len(outs)):
            lag, forward, when = (LAG_DX, None, last) if which % 3 == 2 else (LAG_GRADS, peer, grads)
            made.append((when, functools.partial(out_copy, q, lag, which, forward)))
        if own:
            made += [((q >= LAG_TAPS) & (q < steps + LAG_TAPS), lambda: conv_copy(q)), (grads, lambda: dpre_copy(q))]
        return made

    def at(q, lag, i):
        return (q >= lag) & (q < steps + lag) & (lax.rem(q - lag + pieces, pieces) == i)

    def rowpos(base, k):
        pos = pos_ref[pl.ds(al(base + k * SUB), STRIP), :]
        return jnp.concatenate([pos, pos], axis=1)

    def param(blk, k):
        chip, j = chip_of(blk)
        return par_ref[chip, j, k:k + 1, :]

    def stage_at(q, lag):
        u, i = unit_of(jnp.maximum(q - lag, 0))
        blk, grp = block_of(u)
        return u, i, blk, grp

    zero = lax.div(core, 2)

    def folded(val):
        return jnp.sum(val.reshape(STRIP // SUB, SUB, CH), axis=0)

    def scan_piece(slot, p, back, state):
        first = (p * (PIECE // SUB) + back * (PIECE // SUB - 1)) * SUB
        ahead, stride = first + SUB * back, SUB - 16 * back
        for tt in range(PIECE // SUB):
            decay = ab[slot, pl.ds(al(ahead + tt * stride), SUB), :]
            at_t = pl.ds(al(first + tt * stride + SUB), SUB)
            state = uv[back, slot, at_t, :] + decay * state
            uv[back, slot, at_t, :] = state
            yield 6
        return state

    def products(q):
        u, i, blk, _ = stage_at(q, 0)
        slot, w, us, xs = lax.rem(q, 2), lax.rem(blk, 2), lax.rem(u, 2), lax.rem(u, xslots)
        totals = []
        for src, kind in ((nbuf, 1), (nbuf, 0), (gbuf, 2)):
            total = None
            for k in range(0, DM, KSTEP):
                part = jnp.dot(src[slot, :, k:k + KSTEP], wbuf[w, kind, k:k + KSTEP], preferred_element_type=F32)
                total = part if total is None else total + part
                yield
            if kind == 1:
                total = (total + param(blk, 11)).astype(BF).astype(F32)
                xbuf[xs, pl.ds(al(i * PIECE + HALO), PIECE), :] = total
            totals.append(total)
        yield
        rows = pl.ds(al(i * PIECE, PIECE), PIECE)
        py[us, rows, :] = totals[1] + param(blk, 10)
        dm[us, rows, :] = totals[2]

    def taps(q):
        u, i, blk, grp = stage_at(q, LAG_TAPS)
        base = (i + core * (pieces - 1 - 2 * i)) * PIECE
        xs, cs = lax.rem(u, xslots), lax.rem(q, 2)
        par = [param(blk, k) for k in range(5)]
        for rt in STRIPS:
            pos = rowpos(grp * POS_ROWS + base + rt, 0)
            acc = par[0]
            for k in range(4):
                xk = xbuf[xs, pl.ds(al(base + rt + HALO - SUB * k), STRIP), :]
                if k:
                    xk = jnp.where(pos >= float(k), xk, 0.0)
                acc = acc + xk * par[1 + k]
            conv[cs, rt:rt + STRIP, :] = acc.astype(BF)
            yield 34
        pre[:PIECE] = jnp.dot(conv[cs], wgb[lax.rem(blk, 2)], preferred_element_type=F32)

    def gates(q):
        u, i, blk, grp = stage_at(q, LAG_GATES)
        p = i + core * (pieces - 1 - 2 * i)
        slot, cs = lax.rem(u, 2), lax.rem(q + 1, 2)
        base = p * PIECE
        ba, bi, kh = (param(blk, k) for k in range(5, SUB))
        for rt in STRIPS:
            rd = pl.ds(al(rt + zero * STRIP, STRIP), STRIP)
            rows = pl.ds(al(base + rt, STRIP), STRIP)
            rows8 = pl.ds(al(base + rt + SUB), STRIP)
            v = py[slot, rows, :]
            dmv = dm[slot, rows, :]
            v2 = v * v
            g = 0.5 * jnp.tanh(v * (v2 * GELU_K1 + GELU_K0)) + 0.5
            y = v * g
            yb[slot, rows, :] = y
            w1b[slot, rows, :] = dmv * (g + (v * (g - g * g)) * (v2 * (6.0 * GELU_K1) + 2.0 * GELU_K0))
            uv[1, slot, rows8, :] = dmv * y
            r2 = jnp.tanh(pre[rd, :CH] + ba) + 1.0
            thi = jnp.tanh(pre[rd, CH:] + bi)
            rate = jnp.where(rowpos(grp * POS_ROWS + base + rt, 0) < 0.5, FAR, r2 * kh)
            a = jnp.exp2(rate * -LOG2E)
            msq = jnp.tanh(rate) * (1.0 + a * a)
            rs = lax.rsqrt(jnp.maximum(msq, TINY))
            c = conv[cs, rt:rt + STRIP, :].astype(F32)
            gi = 0.5 * thi + 0.5
            mi = (msq * rs) * gi
            u_in = mi * c
            ab[slot, rows, :] = a
            mib[slot, rows, :] = mi
            uv[0, slot, rows8, :] = u_in
            pb[slot, rows, :] = (gi * c) * (a * rs)
            qab[slot, rows, :] = (a * rate) * (2.0 - r2)
            qib[slot, rows, :] = u_in * (1.0 - thi)
            if own:
                rb[slot, rows, :] = a * r2
            yield 112
        state = yield from scan_piece(slot, p, core, jnp.where(i == 0, 0.0, st1[...]))
        st1[...] = state
        csend[slot] = ab[slot, pl.ds(al(peer * GROWS), SUB), :] * state

    def grads(q):
        _, i, blk, _ = stage_at(q, LAG_GRADS)
        p = i + peer * (pieces - 1 - 2 * i)
        slot = lax.rem(lax.div(q + 3 * pieces - LAG_GRADS, pieces) + 1, 2)
        so = lax.rem(q, 2)
        base = p * PIECE
        entering = enter[...]
        uv[0, slot, pl.ds(0, SUB), :] = jnp.where(core == 1, entering, 0.0)
        st2[...] = yield from scan_piece(slot, p, peer, jnp.where(i == 0, entering, st2[...]))
        sums = [jnp.zeros((SUB, CH), F32)] * 4
        for rt in STRIPS:
            rl = slice(rt, rt + STRIP)
            rows = pl.ds(al(base + rt, STRIP), STRIP)
            rows8 = pl.ds(al(base + rt + SUB), STRIP)
            hid = uv[0, slot, rows8, :]
            dh = uv[1, slot, rows8, :]
            st_m[so, rl, :] = (hid * yb[slot, rows, :]).astype(BF)
            dpy = w1b[slot, rows, :] * hid
            st_y[so, rl, :] = dpy.astype(BF)
            g1 = dh * (pb[slot, rows, :] - uv[0, slot, rows, :])
            dpa = g1 * qab[slot, rows, :]
            dpi = dh * qib[slot, rows, :]
            dconv[rl, :] = dh * mib[slot, rows, :]
            dpre[so, rl, :CH] = dpa.astype(BF)
            dpre[so, rl, CH:] = dpi.astype(BF)
            if own:
                for k, val in enumerate((dpy, dpa, dpi, g1 * rb[slot, rows, :])):
                    sums[k] = sums[k] + folded(val)
            yield 56
        if own:
            for k in range(4):
                stat_ref[blk, k * SUB:k * SUB + SUB, :] += jnp.where(q >= LAG_GRADS, sums[k], 0.0)

    def back(q):
        u, i, blk, grp = stage_at(q, LAG_BACK)
        base = (i + peer * (pieces - 1 - 2 * i)) * PIECE
        slot, so = lax.rem(u, 2), lax.rem(q + 1, 2)
        xs = lax.rem(lax.div(jnp.maximum(q, LAG_BACK - pieces) - LAG_BACK + 4 * pieces, pieces), xslots)
        val = lax.dot_general(dpre[so], wgb[lax.rem(blk, 2)], NT, preferred_element_type=F32)
        dbuf[slot, pl.ds(al(base, PIECE), PIECE), :] = dconv[...] + val
        yield 60
        if own:
            sums = [jnp.zeros((SUB, CH), F32)] * 5
            for rt in STRIPS:
                pos = rowpos(grp * POS_ROWS + base + rt, 0)
                dc = dbuf[slot, pl.ds(al(base + rt, STRIP), STRIP), :]
                sums[0] = sums[0] + folded(dc)
                for k in range(4):
                    xk = xbuf[xs, pl.ds(al(base + rt + HALO - SUB * k), STRIP), :]
                    if k:
                        xk = jnp.where(pos >= float(k), xk, 0.0)
                    sums[1 + k] = sums[1 + k] + folded(dc * xk)
                yield 40
            for k in range(5):
                stat_ref[blk, (5 + k) * SUB:(5 + k) * SUB + SUB, :] += jnp.where(q >= LAG_BACK, sums[k], 0.0)

    def taps_back(q):
        u, i, blk, grp = stage_at(q, LAG_DX)
        slot, so = lax.rem(u, 2), lax.rem(q, 2)
        base = i * PIECE
        par = [param(blk, k) for k in range(1, 5)]
        total = jnp.zeros((SUB, CH), F32)
        for rt in STRIPS:
            acc = dbuf[slot, pl.ds(al(base + rt), STRIP), :] * par[0]
            for k in range(1, 4):
                dk = dbuf[slot, pl.ds(al(base + rt + SUB * k), STRIP), :]
                acc = acc + jnp.where(rowpos(grp * POS_ROWS + base + rt, k) >= float(k), dk, 0.0) * par[k]
            st_x[so, rt:rt + STRIP, :] = acc.astype(BF)
            if own:
                total = total + folded(acc)
            yield 32
        if own:
            stat_ref[blk, 32:40, :] += jnp.where(q >= LAG_DX, total, 0.0)

    def start_of_step(q):
        for when, make in out_copies(q - 2):
            @pl.when(when)
            def _(make=make):
                make().wait()

        @pl.when(at(q, LAG_TAPS, 3) & (core == 0))
        def _():
            halo_copy(lax.div(q - LAG_TAPS, pieces)).wait_send()

        @pl.when(at(q, LAG_TAPS, 3) & (core == 1))
        def _():
            halo_copy(lax.div(q - LAG_TAPS, pieces)).wait_recv()

        @pl.when(at(q, LAG_GRADS, 0))
        def _():
            u = lax.div(q - LAG_GRADS, pieces)
            carry_copy(u).wait()
            enter[...] = crecv[lax.rem(u, 2)]

        @pl.when(at(q, LAG_DX, 3))
        def _():
            dconv_copy(lax.div(q - LAG_DX, pieces)).wait()

        @pl.when((q >= LAG_TAPS) & (q < steps + LAG_TAPS) & (lax.rem(q - LAG_TAPS + groups * pieces, groups * pieces) == 0))
        def _():
            blk = lax.div(q - LAG_TAPS, groups * pieces)
            for cp in gate_copies(blk):
                cp.wait()
            slot = lax.rem(blk, 2)
            wgb[slot, :, :CH] = wgf[slot, 0].astype(BF)
            wgb[slot, :, CH:] = wgf[slot, 1].astype(BF)

            @pl.when(blk + 1 < blocks)
            def _():
                for cp in gate_copies(blk + 1):
                    cp.start()

    def end_of_step(q):
        for when, make in out_copies(q):
            @pl.when(when)
            def _(make=make):
                make().start()

        @pl.when(at(q, LAG_TAPS, 0) & (core == 0))
        def _():
            halo_copy(lax.div(q - LAG_TAPS, pieces)).start()

        @pl.when(at(q, LAG_GATES, 3))
        def _():
            carry_copy(lax.div(q - LAG_GATES, pieces)).start()

        @pl.when(at(q, LAG_BACK, 3))
        def _():
            dconv_copy(lax.div(q - LAG_BACK, pieces)).start()

    for which in range(2):
        row_copy(0, which).start()
    for cp in gate_copies(0):
        cp.start()
    weights_first()
    for slot in range(2):
        ab[slot, pl.ds(GROWS, SUB), :] = jnp.ones((SUB, CH), F32)
    if own:
        stat_ref[...] = jnp.zeros_like(stat_ref)
    barrier = pltpu.get_barrier_semaphore()
    pl.semaphore_signal(barrier, inc=1, device_id={"cp": peer}, device_id_type=pl.DeviceIdType.MESH)
    pl.semaphore_wait(barrier, 1)

    def full_step(q, _):
        for which in range(2):
            row_copy(q, which).wait()

        @pl.when(q + 1 < steps)
        def _():
            for which in range(2):
                row_copy(q + 1, which).start()

        weight_turn(q)
        start_of_step(q)
        product_steps, spent, made = products(q), share, 0
        for stage in (taps_back, back, grads, gates, taps):
            for bundles in stage(q):
                spent += bundles
                while spent >= share and made < 3 * DM // KSTEP:
                    spent -= share
                    made += 1
                    next(product_steps)
        run(product_steps)
        end_of_step(q)
        return 0

    lax.fori_loop(0, steps, full_step, 0)

    def drain_step(q, _):
        start_of_step(q)
        for lag, stage in ((LAG_DX, taps_back), (LAG_BACK, back), (LAG_GRADS, grads), (LAG_GATES, gates), (LAG_TAPS, taps)):
            @pl.when(q < steps + lag)
            def _(stage=stage):
                run(stage(q))
        end_of_step(q)
        return 0

    lax.fori_loop(steps, steps + LAG_DX, drain_step, 0)
    for blk in (blocks - 2, blocks - 1):
        for kind in range(3):
            weight_out(jnp.int32(blk), kind).wait()
    for q in (steps + LAG_DX, steps + LAG_DX + 1):
        for when, make in out_copies(jnp.int32(q - 2)):
            @pl.when(when)
            def _(make=make):
                make().wait()


def rnn_call(phase, groups, n, gz, sources, par, pos, whole):
    own = phase is None
    units = (4 if own else 3) * groups

    def chip_of(blk):
        return (0, blk) if own else (lax.rem(lax.axis_index("tp") + 1 + blk, 4), 0)

    def col_of(blk, merged):
        return lax.axis_index("tp") * 4 + blk if own else chip_of(blk)[0] * 4 + phase

    args = [n, gz, *sources, par, pos, *whole]
    in_specs = [ANY] * (2 + len(sources)) + [VM] * 2 + [ANY] * len(whole)
    out_specs = [ANY] * 4
    out_shape = [sds((ROWS, DM), BF), sds((ROWS, 2 * DM), BF), sds((DM, 2 * DM), BF), sds((DM, DM), BF)]
    alias = {6 + k: k for k in range(len(whole))}
    if own:
        out_specs = [ANY] * 9 + [VM]
        out_shape = out_shape + [sds((ROWS, 4 * CH), BF)] * 3 + [sds((4, ROWS, CH), BF), sds((4, ROWS, 2 * CH), BF), sds((4, 10 * SUB, CH), F32)]

    def buf(slots, rows, dtype=F32, cols=CH):
        return pltpu.VMEM((slots, rows, cols), dtype)

    piece32 = pltpu.VMEM((PIECE, CH), F32)
    scratch = [buf(2, PIECE, BF, DM), buf(2, PIECE, BF, DM), pltpu.VMEM((2, 3, DM, CH), BF), pltpu.VMEM((2, 2, CH, CH), F32), buf(2, CH, BF, 2 * CH),
               buf(2, GROWS), buf(2, GROWS), buf(4 if own else 2, GROWS + HALO), buf(2, GROWS + SUB),
               pltpu.VMEM((2, 2, GROWS + SUB, CH), F32)] + [buf(2, GROWS)] * 6 + [buf(2, GROWS + HALO), buf(2, PIECE, BF),
               pltpu.VMEM((PIECE + STRIP, 2 * CH), F32), buf(2, PIECE, BF, 2 * CH), piece32] + [buf(2, PIECE, BF)] * 3 + [pltpu.VMEM((SUB, CH), F32)] * 3 + [buf(2, SUB)] * 2
    dma = pltpu.SemaphoreType.DMA
    sems = [dma((2,)), dma((2,)), dma((2, 3) if own else (DEPTH,)), dma((2, 3)), dma((2, 2)), dma((6 if own else 3, 2))] + [dma((2,))] * 6
    if own:
        scratch.append(buf(2, GROWS))
        sems.append(dma((2, 2)))
    else:
        scratch.append(buf(DEPTH, WROWS))
    return pl.pallas_call(
        functools.partial(rnn_kernel, own, groups, units, chip_of, col_of), in_specs=in_specs, out_specs=out_specs, out_shape=out_shape,
        scratch_shapes=scratch + sems, input_output_aliases=alias,
        compiler_params=params(collective_id=0 if own else 1 + phase, has_side_effects=True),
        cost_estimate=cost(10 * units))(*args)


def layer(x_in, grad_z, seg_pos, norm_scale, w_x, b_x, w_y, b_y, conv_w, conv_b, w_a, b_a, w_i, b_i, a_param, w_out, b_out):
    core = lax.axis_index("cp")
    swap = [(0, 1), (1, 0)]
    half = core * HALF

    zero = jnp.zeros_like(a_param)
    rows = [conv_b.astype(F32)] + [conv_w[k].astype(F32) for k in range(4)] + [0.5 * b_a.astype(F32), 0.5 * b_i.astype(F32), 4.0 * jax.nn.softplus(a_param), zero, zero,
            b_y.astype(F32), b_x.astype(F32)] + [zero] * 4
    par_own = jnp.stack(rows).reshape(16, 4, CH).transpose(1, 0, 2)
    wg_own = jnp.stack([w_a, w_i], axis=1).astype(F32) * 0.5
    wg_mine = lax.dynamic_index_in_dim(wg_own, core, 1, keepdims=False)

    got = []
    for j in range(4):
        cols = j * CH
        parts = [lax.dynamic_slice(w_y, (half, cols), (HALF, CH)).astype(F32), lax.dynamic_slice(w_x, (half, cols), (HALF, CH)).astype(F32),
                 lax.dynamic_slice(w_out, (cols, half), (CH, HALF)).T.astype(F32), wg_mine[j], par_own[j]]
        mine = lax.optimization_barrier(jnp.concatenate(parts, axis=0))
        got.append(lax.all_gather(mine, "tp"))

    def partner(val):
        return lax.ppermute(val, "cp", swap)

    pos = seg_pos.astype(jnp.int32)
    later = jnp.where(core == 0, partner(pos[:, :SUB]), -1)
    pos = jnp.concatenate([pos, later], axis=1).reshape(GRP, SUB, TOK + SUB).transpose(0, 2, 1).astype(F32)
    pos = jnp.broadcast_to(pos.reshape(GRP * POS_ROWS, 1), (GRP * POS_ROWS, LANES))

    scale = norm_scale.astype(F32)[None]
    n, gz, gb = norm_call(x_in, grad_z, scale)

    first = rnn_call(None, GRP, n, gz, (w_y, w_x, w_out.T, wg_own), par_own[None], pos, ())
    whole, (omixed, ody, odx, conv16, dpre16, stats) = first[:4], first[4:]

    def dot(lhs, rhs, dims):
        return lax.dot_general(lhs, rhs, dims, preferred_element_type=F32)

    for j in range(4):
        other = partner(got[j])
        whole = rnn_call(j, GRP, n, gz, (got[j], other), got[j][:, None, 3 * HALF + CH:], pos, whole)
    mixed, dyx, wyx, wz = whole

    g_w_x = dot(n, odx, TN)
    g_w_y = dot(n, ody, TN)
    g_w_out = dot(omixed, gz, TN)
    g_gate = 0.5 * jnp.einsum("hrk,hrj->hkj", conv16, dpre16, preferred_element_type=F32)
    stats = jnp.sum(stats.reshape(4, 10, SUB, CH), axis=2).transpose(1, 0, 2).reshape(10, 4 * CH)
    g_w_x, g_w_y, g_w_out, g_gate = lax.psum((g_w_x, g_w_y, g_w_out, g_gate), "cp")

    def shared(acts, weight, full):
        own_rows = (ROWS - full) // 4
        mine = lax.dynamic_slice(acts, (full + lax.axis_index("tp") * own_rows, 0), (own_rows, acts.shape[1]))
        mine = lax.optimization_barrier(dot(mine, weight, NT))
        return lax.all_gather(mine, "tp", tiled=True)

    bias = b_out.astype(F32)[None]
    dn_mid, z_mid = FULL_DN // (SUB * TILE), FULL_Z // (SUB * TILE)
    dn_rest, z_rest = shared(dyx, wyx, FULL_DN), shared(mixed, wz, FULL_Z)
    grad_x, gs = gx_call((0, dn_mid), dot(dyx[:FULL_DN], wyx, NT), x_in, grad_z, scale)
    grad_x, gs_rest = gx_call((dn_mid, NBLK), dn_rest, x_in, grad_z, scale, grad_x)
    gs = gs + gs_rest
    z_out = z_call((0, z_mid), dot(mixed[:FULL_Z], wz, NT), x_in, bias)
    z_out = z_call((z_mid, NBLK), z_rest, x_in, bias, z_out)

    sums = jnp.concatenate([jnp.sum(gs, axis=0), stats.reshape(-1), jnp.sum(gb, axis=0)])
    sums = sums + partner(sums)
    g_scale, stats, g_b_out = sums[:DM], sums[DM:-DM].reshape(10, 4 * CH), sums[-DM:]
    return (z_out, grad_x, g_scale, g_w_x, stats[4], g_w_y, stats[0], stats[6:10], stats[5], g_gate[:, :, :CH], 0.5 * stats[1],
            g_gate[:, :, CH:], 0.5 * stats[2], 4.0 * jax.nn.sigmoid(a_param) * stats[3], g_w_out, g_b_out)


def solution(mesh):
    return jax.shard_map(layer, mesh=mesh, in_specs=IN_SPECS, out_specs=OUT_SPECS, check_vma=False)
```

```python
import functools
import jax
import jax.numpy as jnp
from jax import lax
from jax.experimental import pallas as pl
from jax.experimental.pallas import tpu as pltpu
from jax.sharding import PartitionSpec as P

NORM_EPS = 1e-6
TINY, FAR = 1e-37, 1e4
LOG2E = 1.4426950408889634
GELU_K0 = 0.7978845608028654
GELU_K1 = GELU_K0 * 0.044715
SUB = 8
TOK, GRP, CH, DM, LANES, TILE = 128, 4, 256, 4096, 128, 16
GROWS = TOK * SUB
ROWS = GRP * GROWS
HALF = DM // 2
PIECE, HALO, WROWS, DEPTH = 256, 32, 1024, 4
KSTEP, STRIP = 1024, 32
POS_ROWS = GROWS + 64
COLS = DM // LANES
BF, F32 = jnp.bfloat16, jnp.float32
ANY = pl.BlockSpec(memory_space=pl.ANY)
VM = pl.BlockSpec(memory_space=pltpu.VMEM)
VMEM_MOST = 67000000
NT = (((1,), (1,)), ((), ()))
TN = (((0,), (0,)), ((), ()))
SEQ, ALL, CHAN, COL, BLK, ROW = P(None, "cp", None), P(), P("tp"), P(None, "tp"), P("tp", None, None), P("tp", None)
PARAMS = (COL, CHAN, COL, CHAN, COL, CHAN, BLK, CHAN, BLK, CHAN, CHAN, ROW, ALL)
IN_SPECS = (SEQ, SEQ, P(None, "cp"), ALL) + PARAMS
OUT_SPECS = (SEQ, SEQ, ALL) + PARAMS


def sds(shape, dtype):
    return jax.ShapeDtypeStruct(shape, dtype)


def cost(us):
    return pl.CostEstimate(flops=int(us * 1e9), bytes_accessed=int(us * 1e6), transcendentals=0)


def params(**kw):
    return pltpu.CompilerParams(vmem_limit_bytes=VMEM_MOST, **kw)


def lane_tiles():
    return [(j, slice(j * LANES, (j + 1) * LANES)) for j in range(COLS)]


NTOK, WIDE = TOK // TILE, 512
FULL_DN, FULL_Z = 20 * SUB * TILE, 24 * SUB * TILE
NBLK = GRP * NTOK
ONE_ROW = pl.BlockSpec((1, DM), lambda i: (0, 0))
SUM_BLOCK = pl.BlockSpec((SUB, DM), lambda i: (0, 0))
TURN = pltpu.VMEM((COLS, SUB * TILE, LANES), F32)


def seq_block(first):
    return pl.BlockSpec((SUB, TILE, DM), lambda i: ((first + i) // NTOK, (first + i) % NTOK, 0))


def row_call(kernel, us, blocks, inputs, in_specs, out_specs, out_shape, turns, whole=None):
    first, last = blocks
    alias = {}
    if whole is not None:
        alias = {len(inputs): 0}
        inputs = (*inputs, whole)
        in_specs = in_specs + [ANY]
    return pl.pallas_call(kernel, grid=(last - first,), in_specs=in_specs, out_specs=out_specs, out_shape=out_shape, scratch_shapes=[TURN] * turns,
                          input_output_aliases=alias, compiler_params=params(), cost_estimate=cost(us))(*inputs)


def first_step():
    return pl.program_id(0) == 0


def both(val):
    return val[:SUB] + val[SUB:]


def row_scales(x_ref, more=None):
    found = []
    for b in range(SUB):
        square = other = jnp.zeros((TILE, LANES), F32)
        for j, cols in lane_tiles():
            xf = x_ref[b, :, cols].astype(F32)
            square = square + xf * xf
            if more is not None:
                other = other + xf * more(b, j, cols)
        rstd = lax.rsqrt(jnp.sum(square, axis=-1, keepdims=True) * (1.0 / DM) + NORM_EPS)
        found.append((rstd, jnp.sum(other, axis=-1, keepdims=True) * (1.0 / DM)))
    return found


def norm_kernel(x_ref, gz_ref, sc_ref, n_ref, g_ref, gb_ref, sn_ref, sg_ref):
    @pl.when(first_step())
    def _():
        gb_ref[...] = jnp.zeros_like(gb_ref)

    rows = row_scales(x_ref)
    for j, cols in lane_tiles():
        scale = 1.0 + sc_ref[:, cols]
        total = gb_ref[:, cols]
        for b in range(SUB):
            gf = gz_ref[b, :, cols].astype(F32)
            total = total + both(gf)
            sn_ref[j, pl.ds(b, TILE, stride=SUB), :] = x_ref[b, :, cols].astype(F32) * rows[b][0] * scale
            sg_ref[j, pl.ds(b, TILE, stride=SUB), :] = gf
        gb_ref[:, cols] = total
        n_ref[:, cols] = sn_ref[j].astype(BF)
        g_ref[:, cols] = sg_ref[j].astype(BF)


ROW_BLOCK = pl.BlockSpec((SUB * TILE, DM), lambda i: (i, 0))


def norm_call(x, gz, scale):
    seq = seq_block(0)
    return row_call(norm_kernel, 60, (0, NBLK), (x, gz, scale), [seq, seq, ONE_ROW], [ROW_BLOCK, ROW_BLOCK, SUM_BLOCK],
                    [sds((ROWS, DM), BF), sds((ROWS, DM), BF), sds((SUB, DM), F32)], 2)


def z_kernel(acc_ref, x_ref, bo_ref, *refs):
    z_ref, sa_ref = refs[-2:]
    for j, cols in lane_tiles():
        sa_ref[j] = acc_ref[:, cols]
    for b in range(SUB):
        for j, cols in lane_tiles():
            z_ref[b, :, cols] = (x_ref[b, :, cols].astype(F32) + (sa_ref[j, pl.ds(b, TILE, stride=SUB), :] + bo_ref[:, cols])).astype(BF)


def z_call(blocks, acc, x, b_out, whole=None):
    seq = seq_block(blocks[0])
    return row_call(z_kernel, 40, blocks, (acc, x, b_out), [ROW_BLOCK, seq, ONE_ROW], seq, sds((GRP * SUB, TOK, DM), BF), 1, whole)


def proj_kernel(act_ref, w_ref, x_ref, bo_ref, z_ref, sa_ref):
    tok = x_ref.shape[1]
    for half in range(0, WIDE, CH):
        acc = lax.dot_general(act_ref[...], w_ref[half:half + CH], NT, preferred_element_type=F32)
        for j in range(CH // LANES):
            sa_ref[half // LANES + j] = acc[:, j * LANES:(j + 1) * LANES]
    for b in range(SUB):
        for j in range(WIDE // LANES):
            cols = slice(j * LANES, (j + 1) * LANES)
            out = x_ref[b, :, cols].astype(F32) + (sa_ref[j, pl.ds(b, tok, stride=SUB), :] + bo_ref[:, cols])
            z_ref[b, :, cols] = out.astype(BF)


def proj_call(rows, acts, weight, x, b_out):
    tok = WIDE // SUB
    per = TOK // tok
    seq = pl.BlockSpec((SUB, tok, WIDE), lambda n, m: (m // per, m % per, n))
    return pl.pallas_call(
        proj_kernel, grid=(DM // WIDE, rows // WIDE),
        in_specs=[pl.BlockSpec((WIDE, DM), lambda n, m: (m, 0)), pl.BlockSpec((WIDE, DM), lambda n, m: (n, 0)), seq, pl.BlockSpec((1, WIDE), lambda n, m: (0, n))],
        out_specs=seq, out_shape=sds((GRP * SUB, TOK, DM), BF), scratch_shapes=[pltpu.VMEM((WIDE // LANES, WIDE, LANES), F32)],
        compiler_params=params(), cost_estimate=cost(130), name="proj_z")(acts, weight, x, b_out)


def gx_kernel(dn_ref, x_ref, gz_ref, sc_ref, *refs):
    gx_ref, gs_ref, sa_ref = refs[-3:]

    @pl.when(first_step())
    def _():
        gs_ref[...] = jnp.zeros_like(gs_ref)

    for j, cols in lane_tiles():
        sa_ref[j] = dn_ref[:, cols]

    def grad(b, j):
        return sa_ref[j, pl.ds(b, TILE, stride=SUB), :]

    rows = row_scales(x_ref, lambda b, j, cols: grad(b, j) * (1.0 + sc_ref[:, cols]))
    back = [rstd * rstd * rstd * mean for rstd, mean in rows]
    for j, cols in lane_tiles():
        scale = 1.0 + sc_ref[:, cols]
        total = gs_ref[:, cols]
        for b in range(SUB):
            xf = x_ref[b, :, cols].astype(F32)
            dn = grad(b, j) * rows[b][0]
            total = total + both(dn * xf)
            gx_ref[b, :, cols] = (gz_ref[b, :, cols].astype(F32) + (dn * scale - xf * back[b])).astype(BF)
        gs_ref[:, cols] = total


def gx_call(blocks, dn, x, gz, scale, whole=None):
    seq = seq_block(blocks[0])
    return row_call(gx_kernel, 50, blocks, (dn, x, gz, scale), [ROW_BLOCK, seq, seq, ONE_ROW], [seq, SUM_BLOCK],
                    [sds((GRP * SUB, TOK, DM), BF), sds((SUB, DM), F32)], 1, whole)


def run(steps):
    for _ in steps:
        pass


LAG_TAPS, LAG_GATES, LAG_GRADS, LAG_BACK, LAG_DX = 4, 5, 10, 11, 15
STRIPS = tuple(range(0, PIECE, STRIP))


def rnn_kernel(own, groups, units, chip_of, col_of, *refs):
    it = iter(refs)

    def take(count):
        return [next(it) for _ in range(count)]

    n_hbm, g_hbm = take(2)
    if own:
        own_w = take(3)
        gate_hbm = take(1)
    else:
        gate_hbm = take(2)
    par_ref, pos_ref = take(2)
    if not own:
        take(4)
    mixed_hbm, dyx_hbm, wyx_hbm, wz_hbm = take(4)
    outs = [mixed_hbm, dyx_hbm, dyx_hbm]
    if own:
        outs += take(3)
        conv_hbm, dpre_hbm, stat_ref = take(3)
    nbuf, gbuf, wbuf, wgf, wgb, py, dm, xbuf, ab, uv, yb, w1b, pb, qab, qib, mib, dbuf, conv, pre, dpre, dconv, st_m, st_y, st_x, st1, st2, enter, csend, crecv = take(29)
    if own:
        rb = next(it)
    if not own:
        stage = next(it)
    n_sem, g_sem, w_sem, wo_sem, wg_sem, o_sem, c_send, c_recv, d_send, d_recv, x_send, x_recv = take(12)
    if own:
        p_sem = next(it)

    core = lax.axis_index("cp")
    peer = 1 - core
    pieces = GROWS // PIECE
    steps = units * pieces
    xslots = xbuf.shape[0]
    share = 220 if own else 180

    def unit_of(q):
        return lax.div(q, pieces), lax.rem(q, pieces)

    def block_of(u):
        return lax.div(u, groups), lax.rem(u, groups)

    def al(val, mult=SUB):
        return pl.multiple_of(val, mult)

    def row_copy(q, which):
        u, i = unit_of(q)
        rows = pl.ds(al(block_of(u)[1] * GROWS + i * PIECE, PIECE), PIECE)
        slot = lax.rem(q, 2)
        src, dst, sem = ((n_hbm, nbuf, n_sem), (g_hbm, gbuf, g_sem))[which]
        return pltpu.make_async_copy(src.at[rows], dst.at[slot], sem.at[slot])

    blocks, turns = units // groups, groups * pieces

    def weight_in(blk, kind):
        slot = lax.rem(blk, 2)
        return pltpu.make_async_copy(own_w[kind].at[:, pl.ds(al(blk * CH, CH), CH)], wbuf.at[slot, kind], w_sem.at[slot, kind])

    def weight_out(blk, kind):
        slot = lax.rem(blk, 2)
        col = col_of(blk, True) * CH + (DM if kind == 1 else 0)
        dst = wz_hbm if kind == 2 else wyx_hbm
        return pltpu.make_async_copy(wbuf.at[slot, kind], dst.at[:, pl.ds(al(col, CH), CH)], wo_sem.at[slot, kind])

    per_half = 3 * HALF // WROWS

    def strip_slot(t, half):
        return lax.rem(t + half * per_half, DEPTH)

    def strip_in(blk, t, half):
        rows = pl.ds(al(t * WROWS, WROWS), WROWS)
        return pltpu.make_async_copy(gate_hbm[half].at[chip_of(blk)[0], rows], stage.at[strip_slot(t, half)], w_sem.at[strip_slot(t, half)])

    def strip_cast(blk, t, half):
        per_kind = HALF // WROWS
        row = (peer if half else core) * HALF + lax.rem(t, per_kind) * WROWS
        wbuf[lax.rem(blk, 2), lax.div(t, per_kind), pl.ds(al(row, WROWS), WROWS), :] = stage[strip_slot(t, half)].astype(BF)

    def weight_turn(q):
        blk, t = lax.div(q, turns), lax.rem(q, turns)

        @pl.when((t == 0) & (blk >= 1) & (blk + 1 < blocks))
        def _():
            for kind in range(3):
                weight_out(blk - 1, kind).wait()

        if own:
            @pl.when(t == 0)
            def _():
                for kind in range(3):
                    weight_in(blk, kind).wait()
                    weight_out(blk, kind).start()

                @pl.when(blk + 1 < blocks)
                def _():
                    for kind in range(3):
                        weight_in(blk + 1, kind).start()

            return
        more = blk + 1 < blocks
        for half in range(2):
            done = t - 1 - half * per_half

            @pl.when(more & (done >= 0) & (done < per_half))
            def _(half=half, done=done):
                strip_in(blk + 1, done, half).wait()
                strip_cast(blk + 1, done, half)
        for half in range(2):
            new = t - half * per_half

            @pl.when(more & (new >= 0) & (new < per_half))
            def _(half=half, new=new):
                strip_in(blk + 1, new, half).start()

        @pl.when(more & (t == 2 * per_half + 1))
        def _():
            for kind in range(3):
                weight_out(blk + 1, kind).start()

    def weights_first():
        if own:
            for kind in range(3):
                weight_in(0, kind).start()
            return
        ahead = DEPTH - 1
        for t in range(ahead):
            strip_in(0, t, 0).start()
        for half in range(2):
            def turn(t, _, half=half):
                @pl.when(t + ahead < per_half)
                def _():
                    strip_in(0, t + ahead, half).start()

                if half == 0:
                    @pl.when(t + ahead >= per_half)
                    def _():
                        strip_in(0, t + ahead - per_half, 1).start()
                strip_in(0, t, half).wait()
                strip_cast(0, t, half)
                return 0

            lax.fori_loop(0, per_half, turn, 0)
        for kind in range(3):
            weight_out(0, kind).start()

    def gate_copies(blk):
        slot = lax.rem(blk, 2)
        chip, j = chip_of(blk)
        if own:
            return [pltpu.make_async_copy(gate_hbm[0].at[j], wgf.at[slot], wg_sem.at[0, slot])]
        rows = pl.ds(3 * HALF, CH)
        return [pltpu.make_async_copy(gate_hbm[w].at[chip, rows], wgf.at[slot, (peer if w else core)], wg_sem.at[w, slot]) for w in range(2)]

    def out_copy(q, lag, which, forward):
        u, i = unit_of(q - lag)
        blk, grp = block_of(u)
        p = i if forward is None else i + forward * (pieces - 1 - 2 * i)
        slot = lax.rem(q, 2)
        src = (st_m, st_y, st_x)[which % 3].at[slot]
        rows = pl.ds(al(grp * GROWS + p * PIECE, PIECE), PIECE)
        col = blk if which >= 3 else col_of(blk, True) + (DM // CH if which == 2 else 0)
        return pltpu.make_async_copy(src, outs[which].at[rows, pl.ds(al(col * CH, CH), CH)], o_sem.at[which, slot])

    def conv_copy(q):
        u, i = unit_of(q - LAG_TAPS)
        blk, grp = block_of(u)
        p = i + core * (pieces - 1 - 2 * i)
        slot = lax.rem(q, 2)
        rows = pl.ds(al(grp * GROWS + p * PIECE, PIECE), PIECE)
        return pltpu.make_async_copy(conv.at[slot], conv_hbm.at[blk, rows], p_sem.at[0, slot])

    def dpre_copy(q):
        u, i = unit_of(q - LAG_GRADS)
        blk, grp = block_of(u)
        p = i + peer * (pieces - 1 - 2 * i)
        slot = lax.rem(q, 2)
        rows = pl.ds(al(grp * GROWS + p * PIECE, PIECE), PIECE)
        return pltpu.make_async_copy(dpre.at[slot], dpre_hbm.at[blk, rows], p_sem.at[1, slot])

    def remote(src, dst, send, recv):
        return pltpu.make_async_remote_copy(src_ref=src, dst_ref=dst, send_sem=send, recv_sem=recv, device_id={"cp": peer}, device_id_type=pl.DeviceIdType.MESH)

    def halo_copy(u):
        slot, sem = lax.rem(u, xslots), lax.rem(u, 2)
        return remote(xbuf.at[slot, pl.ds(HALO + GROWS - 24, 24)], xbuf.at[slot, pl.ds(HALO - 24, 24)], x_send.at[sem], x_recv.at[sem])

    def carry_copy(u):
        slot = lax.rem(u, 2)
        return remote(csend.at[slot], crecv.at[slot], c_send.at[slot], c_recv.at[slot])

    def dconv_copy(u):
        slot = lax.rem(u, 2)
        return remote(dbuf.at[slot, pl.ds(0, 24)], dbuf.at[slot, pl.ds(GROWS, 24)], d_send.at[slot], d_recv.at[slot])

    def out_copies(q):
        grads = (q >= LAG_GRADS) & (q < steps + LAG_GRADS)
        last = (q >= LAG_DX) & (q < steps + LAG_DX)
        made = []
        for which in range(len(outs)):
            lag, forward, when = (LAG_DX, None, last) if which % 3 == 2 else (LAG_GRADS, peer, grads)
            made.append((when, functools.partial(out_copy, q, lag, which, forward)))
        if own:
            made += [((q >= LAG_TAPS) & (q < steps + LAG_TAPS), lambda: conv_copy(q)), (grads, lambda: dpre_copy(q))]
        return made

    def at(q, lag, i):
        return (q >= lag) & (q < steps + lag) & (lax.rem(q - lag + pieces, pieces) == i)

    def rowpos(base, k):
        pos = pos_ref[pl.ds(al(base + k * SUB), STRIP), :]
        return jnp.concatenate([pos, pos], axis=1)

    def param(blk, k):
        chip, j = chip_of(blk)
        return par_ref[chip, j, k:k + 1, :]

    def stage_at(q, lag):
        u, i = unit_of(jnp.maximum(q - lag, 0))
        blk, grp = block_of(u)
        return u, i, blk, grp

    zero = lax.div(core, 2)

    def folded(val):
        return jnp.sum(val.reshape(STRIP // SUB, SUB, CH), axis=0)

    def scan_piece(slot, p, back, state):
        first = (p * (PIECE // SUB) + back * (PIECE // SUB - 1)) * SUB
        ahead, stride = first + SUB * back, SUB - 16 * back
        for tt in range(PIECE // SUB):
            decay = ab[slot, pl.ds(al(ahead + tt * stride), SUB), :]
            at_t = pl.ds(al(first + tt * stride + SUB), SUB)
            state = uv[back, slot, at_t, :] + decay * state
            uv[back, slot, at_t, :] = state
            yield 6
        return state

    def products(q):
        u, i, blk, _ = stage_at(q, 0)
        slot, w, us, xs = lax.rem(q, 2), lax.rem(blk, 2), lax.rem(u, 2), lax.rem(u, xslots)
        totals = []
        for src, kind in ((nbuf, 1), (nbuf, 0), (gbuf, 2)):
            total = None
            for k in range(0, DM, KSTEP):
                part = jnp.dot(src[slot, :, k:k + KSTEP], wbuf[w, kind, k:k + KSTEP], preferred_element_type=F32)
                total = part if total is None else total + part
                yield
            if kind == 1:
                total = (total + param(blk, 11)).astype(BF).astype(F32)
                xbuf[xs, pl.ds(al(i * PIECE + HALO), PIECE), :] = total
            totals.append(total)
        yield
        rows = pl.ds(al(i * PIECE, PIECE), PIECE)
        py[us, rows, :] = totals[1] + param(blk, 10)
        dm[us, rows, :] = totals[2]

    def taps(q):
        u, i, blk, grp = stage_at(q, LAG_TAPS)
        base = (i + core * (pieces - 1 - 2 * i)) * PIECE
        xs, cs = lax.rem(u, xslots), lax.rem(q, 2)
        par = [param(blk, k) for k in range(5)]
        for rt in STRIPS:
            pos = rowpos(grp * POS_ROWS + base + rt, 0)
            acc = par[0]
            for k in range(4):
                xk = xbuf[xs, pl.ds(al(base + rt + HALO - SUB * k), STRIP), :]
                if k:
                    xk = jnp.where(pos >= float(k), xk, 0.0)
                acc = acc + xk * par[1 + k]
            conv[cs, rt:rt + STRIP, :] = acc.astype(BF)
            yield 34
        pre[:PIECE] = jnp.dot(conv[cs], wgb[lax.rem(blk, 2)], preferred_element_type=F32)

    def gates(q):
        u, i, blk, grp = stage_at(q, LAG_GATES)
        p = i + core * (pieces - 1 - 2 * i)
        slot, cs = lax.rem(u, 2), lax.rem(q + 1, 2)
        base = p * PIECE
        ba, bi, kh = (param(blk, k) for k in range(5, SUB))
        for rt in STRIPS:
            rd = pl.ds(al(rt + zero * STRIP, STRIP), STRIP)
            rows = pl.ds(al(base + rt, STRIP), STRIP)
            rows8 = pl.ds(al(base + rt + SUB), STRIP)
            v = py[slot, rows, :]
            dmv = dm[slot, rows, :]
            v2 = v * v
            g = 0.5 * jnp.tanh(v * (v2 * GELU_K1 + GELU_K0)) + 0.5
            y = v * g
            yb[slot, rows, :] = y
            w1b[slot, rows, :] = dmv * (g + (v * (g - g * g)) * (v2 * (6.0 * GELU_K1) + 2.0 * GELU_K0))
            uv[1, slot, rows8, :] = dmv * y
            r2 = jnp.tanh(pre[rd, :CH] + ba) + 1.0
            thi = jnp.tanh(pre[rd, CH:] + bi)
            rate = jnp.where(rowpos(grp * POS_ROWS + base + rt, 0) < 0.5, FAR, r2 * kh)
            a = jnp.exp2(rate * -LOG2E)
            msq = jnp.tanh(rate) * (1.0 + a * a)
            rs = lax.rsqrt(jnp.maximum(msq, TINY))
            c = conv[cs, rt:rt + STRIP, :].astype(F32)
            gi = 0.5 * thi + 0.5
            mi = (msq * rs) * gi
            u_in = mi * c
            ab[slot, rows, :] = a
            mib[slot, rows, :] = mi
            uv[0, slot, rows8, :] = u_in
            pb[slot, rows, :] = (gi * c) * (a * rs)
            qab[slot, rows, :] = (a * rate) * (2.0 - r2)
            qib[slot, rows, :] = u_in * (1.0 - thi)
            if own:
                rb[slot, rows, :] = a * r2
            yield 112
        state = yield from scan_piece(slot, p, core, jnp.where(i == 0, 0.0, st1[...]))
        st1[...] = state
        csend[slot] = ab[slot, pl.ds(al(peer * GROWS), SUB), :] * state

    def grads(q):
        _, i, blk, _ = stage_at(q, LAG_GRADS)
        p = i + peer * (pieces - 1 - 2 * i)
        slot = lax.rem(lax.div(q + 3 * pieces - LAG_GRADS, pieces) + 1, 2)
        so = lax.rem(q, 2)
        base = p * PIECE
        entering = enter[...]
        uv[0, slot, pl.ds(0, SUB), :] = jnp.where(core == 1, entering, 0.0)
        st2[...] = yield from scan_piece(slot, p, peer, jnp.where(i == 0, entering, st2[...]))
        sums = [jnp.zeros((SUB, CH), F32)] * 4
        for rt in STRIPS:
            rl = slice(rt, rt + STRIP)
            rows = pl.ds(al(base + rt, STRIP), STRIP)
            rows8 = pl.ds(al(base + rt + SUB), STRIP)
            hid = uv[0, slot, rows8, :]
            dh = uv[1, slot, rows8, :]
            st_m[so, rl, :] = (hid * yb[slot, rows, :]).astype(BF)
            dpy = w1b[slot, rows, :] * hid
            st_y[so, rl, :] = dpy.astype(BF)
            g1 = dh * (pb[slot, rows, :] - uv[0, slot, rows, :])
            dpa = g1 * qab[slot, rows, :]
            dpi = dh * qib[slot, rows, :]
            dconv[rl, :] = dh * mib[slot, rows, :]
            dpre[so, rl, :CH] = dpa.astype(BF)
            dpre[so, rl, CH:] = dpi.astype(BF)
            if own:
                for k, val in enumerate((dpy, dpa, dpi, g1 * rb[slot, rows, :])):
                    sums[k] = sums[k] + folded(val)
            yield 56
        if own:
            for k in range(4):
                stat_ref[blk, k * SUB:k * SUB + SUB, :] += jnp.where(q >= LAG_GRADS, sums[k], 0.0)

    def back(q):
        u, i, blk, grp = stage_at(q, LAG_BACK)
        base = (i + peer * (pieces - 1 - 2 * i)) * PIECE
        slot, so = lax.rem(u, 2), lax.rem(q + 1, 2)
        xs = lax.rem(lax.div(jnp.maximum(q, LAG_BACK - pieces) - LAG_BACK + 4 * pieces, pieces), xslots)
        val = lax.dot_general(dpre[so], wgb[lax.rem(blk, 2)], NT, preferred_element_type=F32)
        dbuf[slot, pl.ds(al(base, PIECE), PIECE), :] = dconv[...] + val
        yield 60
        if own:
            sums = [jnp.zeros((SUB, CH), F32)] * 5
            for rt in STRIPS:
                pos = rowpos(grp * POS_ROWS + base + rt, 0)
                dc = dbuf[slot, pl.ds(al(base + rt, STRIP), STRIP), :]
                sums[0] = sums[0] + folded(dc)
                for k in range(4):
                    xk = xbuf[xs, pl.ds(al(base + rt + HALO - SUB * k), STRIP), :]
                    if k:
                        xk = jnp.where(pos >= float(k), xk, 0.0)
                    sums[1 + k] = sums[1 + k] + folded(dc * xk)
                yield 40
            for k in range(5):
                stat_ref[blk, (5 + k) * SUB:(5 + k) * SUB + SUB, :] += jnp.where(q >= LAG_BACK, sums[k], 0.0)

    def taps_back(q):
        u, i, blk, grp = stage_at(q, LAG_DX)
        slot, so = lax.rem(u, 2), lax.rem(q, 2)
        base = i * PIECE
        par = [param(blk, k) for k in range(1, 5)]
        total = jnp.zeros((SUB, CH), F32)
        for rt in STRIPS:
            acc = dbuf[slot, pl.ds(al(base + rt), STRIP), :] * par[0]
            for k in range(1, 4):
                dk = dbuf[slot, pl.ds(al(base + rt + SUB * k), STRIP), :]
                acc = acc + jnp.where(rowpos(grp * POS_ROWS + base + rt, k) >= float(k), dk, 0.0) * par[k]
            st_x[so, rt:rt + STRIP, :] = acc.astype(BF)
            if own:
                total = total + folded(acc)
            yield 32
        if own:
            stat_ref[blk, 32:40, :] += jnp.where(q >= LAG_DX, total, 0.0)

    def start_of_step(q):
        for when, make in out_copies(q - 2):
            @pl.when(when)
            def _(make=make):
                make().wait()

        @pl.when(at(q, LAG_TAPS, 3) & (core == 0))
        def _():
            halo_copy(lax.div(q - LAG_TAPS, pieces)).wait_send()

        @pl.when(at(q, LAG_TAPS, 3) & (core == 1))
        def _():
            halo_copy(lax.div(q - LAG_TAPS, pieces)).wait_recv()

        @pl.when(at(q, LAG_GRADS, 0))
        def _():
            u = lax.div(q - LAG_GRADS, pieces)
            carry_copy(u).wait()
            enter[...] = crecv[lax.rem(u, 2)]

        @pl.when(at(q, LAG_DX, 3))
        def _():
            dconv_copy(lax.div(q - LAG_DX, pieces)).wait()

        @pl.when((q >= LAG_TAPS) & (q < steps + LAG_TAPS) & (lax.rem(q - LAG_TAPS + groups * pieces, groups * pieces) == 0))
        def _():
            blk = lax.div(q - LAG_TAPS, groups * pieces)
            for cp in gate_copies(blk):
                cp.wait()
            slot = lax.rem(blk, 2)
            wgb[slot, :, :CH] = wgf[slot, 0].astype(BF)
            wgb[slot, :, CH:] = wgf[slot, 1].astype(BF)

            @pl.when(blk + 1 < blocks)
            def _():
                for cp in gate_copies(blk + 1):
                    cp.start()

    def end_of_step(q):
        for when, make in out_copies(q):
            @pl.when(when)
            def _(make=make):
                make().start()

        @pl.when(at(q, LAG_TAPS, 0) & (core == 0))
        def _():
            halo_copy(lax.div(q - LAG_TAPS, pieces)).start()

        @pl.when(at(q, LAG_GATES, 3))
        def _():
            carry_copy(lax.div(q - LAG_GATES, pieces)).start()

        @pl.when(at(q, LAG_BACK, 3))
        def _():
            dconv_copy(lax.div(q - LAG_BACK, pieces)).start()

    for which in range(2):
        row_copy(0, which).start()
    for cp in gate_copies(0):
        cp.start()
    weights_first()
    for slot in range(2):
        ab[slot, pl.ds(GROWS, SUB), :] = jnp.ones((SUB, CH), F32)
    if own:
        stat_ref[...] = jnp.zeros_like(stat_ref)
    barrier = pltpu.get_barrier_semaphore()
    pl.semaphore_signal(barrier, inc=1, device_id={"cp": peer}, device_id_type=pl.DeviceIdType.MESH)
    pl.semaphore_wait(barrier, 1)

    def full_step(q, _):
        for which in range(2):
            row_copy(q, which).wait()

        @pl.when(q + 1 < steps)
        def _():
            for which in range(2):
                row_copy(q + 1, which).start()

        weight_turn(q)
        start_of_step(q)
        product_steps, spent, made = products(q), share, 0
        for stage in (taps_back, back, grads, gates, taps):
            for bundles in stage(q):
                spent += bundles
                while spent >= share and made < 3 * DM // KSTEP:
                    spent -= share
                    made += 1
                    next(product_steps)
        run(product_steps)
        end_of_step(q)
        return 0

    lax.fori_loop(0, steps, full_step, 0)

    def drain_step(q, _):
        start_of_step(q)
        for lag, stage in ((LAG_DX, taps_back), (LAG_BACK, back), (LAG_GRADS, grads), (LAG_GATES, gates), (LAG_TAPS, taps)):
            @pl.when(q < steps + lag)
            def _(stage=stage):
                run(stage(q))
        end_of_step(q)
        return 0

    lax.fori_loop(steps, steps + LAG_DX, drain_step, 0)
    for blk in (blocks - 2, blocks - 1):
        for kind in range(3):
            weight_out(jnp.int32(blk), kind).wait()
    for q in (steps + LAG_DX, steps + LAG_DX + 1):
        for when, make in out_copies(jnp.int32(q - 2)):
            @pl.when(when)
            def _(make=make):
                make().wait()


def rnn_call(phase, groups, n, gz, sources, par, pos, whole):
    own = phase is None
    units = (4 if own else 3) * groups

    def chip_of(blk):
        return (0, blk) if own else (lax.rem(lax.axis_index("tp") + 1 + blk, 4), 0)

    def col_of(blk, merged):
        return lax.axis_index("tp") * 4 + blk if own else chip_of(blk)[0] * 4 + phase

    args = [n, gz, *sources, par, pos, *whole]
    in_specs = [ANY] * (2 + len(sources)) + [VM] * 2 + [ANY] * len(whole)
    out_specs = [ANY] * 4
    out_shape = [sds((ROWS, DM), BF), sds((ROWS, 2 * DM), BF), sds((DM, 2 * DM), BF), sds((DM, DM), BF)]
    alias = {6 + k: k for k in range(len(whole))}
    if own:
        out_specs = [ANY] * 9 + [VM]
        out_shape = out_shape + [sds((ROWS, 4 * CH), BF)] * 3 + [sds((4, ROWS, CH), BF), sds((4, ROWS, 2 * CH), BF), sds((4, 10 * SUB, CH), F32)]

    def buf(slots, rows, dtype=F32, cols=CH):
        return pltpu.VMEM((slots, rows, cols), dtype)

    piece32 = pltpu.VMEM((PIECE, CH), F32)
    scratch = [buf(2, PIECE, BF, DM), buf(2, PIECE, BF, DM), pltpu.VMEM((2, 3, DM, CH), BF), pltpu.VMEM((2, 2, CH, CH), F32), buf(2, CH, BF, 2 * CH),
               buf(2, GROWS), buf(2, GROWS), buf(4 if own else 2, GROWS + HALO), buf(2, GROWS + SUB),
               pltpu.VMEM((2, 2, GROWS + SUB, CH), F32)] + [buf(2, GROWS)] * 6 + [buf(2, GROWS + HALO), buf(2, PIECE, BF),
               pltpu.VMEM((PIECE + STRIP, 2 * CH), F32), buf(2, PIECE, BF, 2 * CH), piece32] + [buf(2, PIECE, BF)] * 3 + [pltpu.VMEM((SUB, CH), F32)] * 3 + [buf(2, SUB)] * 2
    dma = pltpu.SemaphoreType.DMA
    sems = [dma((2,)), dma((2,)), dma((2, 3) if own else (DEPTH,)), dma((2, 3)), dma((2, 2)), dma((6 if own else 3, 2))] + [dma((2,))] * 6
    if own:
        scratch.append(buf(2, GROWS))
        sems.append(dma((2, 2)))
    else:
        scratch.append(buf(DEPTH, WROWS))
    return pl.pallas_call(
        functools.partial(rnn_kernel, own, groups, units, chip_of, col_of), in_specs=in_specs, out_specs=out_specs, out_shape=out_shape,
        scratch_shapes=scratch + sems, input_output_aliases=alias,
        compiler_params=params(collective_id=0 if own else 1 + phase, has_side_effects=True),
        cost_estimate=cost(10 * units))(*args)


def layer(x_in, grad_z, seg_pos, norm_scale, w_x, b_x, w_y, b_y, conv_w, conv_b, w_a, b_a, w_i, b_i, a_param, w_out, b_out):
    core = lax.axis_index("cp")
    swap = [(0, 1), (1, 0)]
    half = core * HALF

    zero = jnp.zeros_like(a_param)
    rows = [conv_b.astype(F32)] + [conv_w[k].astype(F32) for k in range(4)] + [0.5 * b_a.astype(F32), 0.5 * b_i.astype(F32), 4.0 * jax.nn.softplus(a_param), zero, zero,
            b_y.astype(F32), b_x.astype(F32)] + [zero] * 4
    par_own = jnp.stack(rows).reshape(16, 4, CH).transpose(1, 0, 2)
    wg_own = jnp.stack([w_a, w_i], axis=1).astype(F32) * 0.5
    wg_mine = lax.dynamic_index_in_dim(wg_own, core, 1, keepdims=False)

    got = []
    for j in range(4):
        cols = j * CH
        rows_out = lax.dynamic_slice(w_out, (cols, half), (CH, HALF))
        if j == 0:
            rows_out = lax.optimization_barrier(rows_out)
        parts = [lax.dynamic_slice(w_y, (half, cols), (HALF, CH)).astype(F32), lax.dynamic_slice(w_x, (half, cols), (HALF, CH)).astype(F32),
                 rows_out.T.astype(F32), wg_mine[j], par_own[j]]
        mine = lax.optimization_barrier(jnp.concatenate(parts, axis=0))
        got.append(lax.all_gather(mine, "tp"))

    def partner(val):
        return lax.ppermute(val, "cp", swap)

    pos = seg_pos.astype(jnp.int32)
    later = jnp.where(core == 0, partner(pos[:, :SUB]), -1)
    pos = jnp.concatenate([pos, later], axis=1).reshape(GRP, SUB, TOK + SUB).transpose(0, 2, 1).astype(F32)
    pos = jnp.broadcast_to(pos.reshape(GRP * POS_ROWS, 1), (GRP * POS_ROWS, LANES))

    scale = norm_scale.astype(F32)[None]
    n, gz, gb = norm_call(x_in, grad_z, scale)

    first = rnn_call(None, GRP, n, gz, (w_y, w_x, w_out.T, wg_own), par_own[None], pos, ())
    whole, (omixed, ody, odx, conv16, dpre16, stats) = first[:4], first[4:]

    def dot(lhs, rhs, dims):
        return lax.dot_general(lhs, rhs, dims, preferred_element_type=F32)

    for j in range(4):
        other = partner(got[j])
        whole = rnn_call(j, GRP, n, gz, (got[j], other), got[j][:, None, 3 * HALF + CH:], pos, whole)
    mixed, dyx, wyx, wz = whole

    g_w_x = dot(n, odx, TN)
    g_w_y = dot(n, ody, TN)
    g_w_out = dot(omixed, gz, TN)
    g_gate = 0.5 * jnp.einsum("hrk,hrj->hkj", conv16, dpre16, preferred_element_type=F32)
    stats = jnp.sum(stats.reshape(4, 10, SUB, CH), axis=2).transpose(1, 0, 2).reshape(10, 4 * CH)

    def merged(val):
        theirs = partner(val)
        return val + theirs

    g_w_x, g_w_y, g_w_out, g_gate = merged(g_w_x), merged(g_w_y), merged(g_w_out), merged(g_gate)

    def shared(acts, weight, full):
        own_rows = (ROWS - full) // 4
        mine = lax.dynamic_slice(acts, (full + lax.axis_index("tp") * own_rows, 0), (own_rows, acts.shape[1]))
        mine = lax.optimization_barrier(dot(mine, weight, NT))
        return lax.all_gather(mine, "tp", tiled=True)

    bias = b_out.astype(F32)[None]
    dn_mid, z_mid = FULL_DN // (SUB * TILE), FULL_Z // (SUB * TILE)
    dn_rest, z_rest = shared(dyx, wyx, FULL_DN), shared(mixed, wz, FULL_Z)
    grad_x, gs = gx_call((0, dn_mid), dot(dyx[:FULL_DN], wyx, NT), x_in, grad_z, scale)
    grad_x, gs_rest = gx_call((dn_mid, NBLK), dn_rest, x_in, grad_z, scale, grad_x)
    gs = gs + gs_rest
    z_out = proj_call(FULL_Z, mixed, wz, x_in, bias)
    z_out = z_call((z_mid, NBLK), z_rest, x_in, bias, z_out)

    sums = jnp.concatenate([jnp.sum(gs, axis=0), stats.reshape(-1), jnp.sum(gb, axis=0)])
    sums = merged(sums)
    g_scale, stats, g_b_out = sums[:DM], sums[DM:-DM].reshape(10, 4 * CH), sums[-DM:]
    return (z_out, grad_x, g_scale, g_w_x, stats[4], g_w_y, stats[0], stats[6:10], stats[5], g_gate[:, :, :CH], 0.5 * stats[1],
            g_gate[:, :, CH:], 0.5 * stats[2], 4.0 * jax.nn.sigmoid(a_param) * stats[3], g_w_out, g_b_out)


def solution(mesh):
    return jax.shard_map(layer, mesh=mesh, in_specs=IN_SPECS, out_specs=OUT_SPECS, check_vma=False)
```

```python
import functools
import jax
import jax.numpy as jnp
from jax import lax
from jax.experimental import pallas as pl
from jax.experimental.pallas import tpu as pltpu
from jax.sharding import PartitionSpec as P

NORM_EPS = 1e-6
TINY, FAR = 1e-37, 1e4
LOG2E = 1.4426950408889634
GELU_K0 = 0.7978845608028654
GELU_K1 = GELU_K0 * 0.044715
SUB = 8
TOK, GRP, CH, DM, LANES, TILE = 128, 4, 256, 4096, 128, 16
GROWS = TOK * SUB
ROWS = GRP * GROWS
HALF = DM // 2
PIECE, HALO, WROWS, DEPTH = 256, 32, 1024, 4
KSTEP, STRIP = 1024, 32
POS_ROWS = GROWS + 64
COLS = DM // LANES
BF, F32 = jnp.bfloat16, jnp.float32
ANY = pl.BlockSpec(memory_space=pl.ANY)
VM = pl.BlockSpec(memory_space=pltpu.VMEM)
VMEM_MOST = 67000000
NT = (((1,), (1,)), ((), ()))
TN = (((0,), (0,)), ((), ()))
SEQ, ALL, CHAN, COL, BLK, ROW = P(None, "cp", None), P(), P("tp"), P(None, "tp"), P("tp", None, None), P("tp", None)
PARAMS = (COL, CHAN, COL, CHAN, COL, CHAN, BLK, CHAN, BLK, CHAN, CHAN, ROW, ALL)
IN_SPECS = (SEQ, SEQ, P(None, "cp"), ALL) + PARAMS
OUT_SPECS = (SEQ, SEQ, ALL) + PARAMS


def sds(shape, dtype):
    return jax.ShapeDtypeStruct(shape, dtype)


def cost(us):
    return pl.CostEstimate(flops=int(us * 1e9), bytes_accessed=int(us * 1e6), transcendentals=0)


def params(**kw):
    return pltpu.CompilerParams(vmem_limit_bytes=VMEM_MOST, **kw)


def lane_tiles():
    return [(j, slice(j * LANES, (j + 1) * LANES)) for j in range(COLS)]


NTOK, WIDE = TOK // TILE, 512
FULL_DN, FULL_Z = 18 * SUB * TILE, 24 * SUB * TILE
NBLK = GRP * NTOK
ONE_ROW = pl.BlockSpec((1, DM), lambda i: (0, 0))
SUM_BLOCK = pl.BlockSpec((SUB, DM), lambda i: (0, 0))
TURN = pltpu.VMEM((COLS, SUB * TILE, LANES), F32)


def seq_block(first):
    return pl.BlockSpec((SUB, TILE, DM), lambda i: ((first + i) // NTOK, (first + i) % NTOK, 0))


def row_call(kernel, us, blocks, inputs, in_specs, out_specs, out_shape, turns, whole=None):
    first, last = blocks
    alias = {}
    if whole is not None:
        alias = {len(inputs): 0}
        inputs = (*inputs, whole)
        in_specs = in_specs + [ANY]
    return pl.pallas_call(kernel, grid=(last - first,), in_specs=in_specs, out_specs=out_specs, out_shape=out_shape, scratch_shapes=[TURN] * turns,
                          input_output_aliases=alias, compiler_params=params(), cost_estimate=cost(us))(*inputs)


def first_step():
    return pl.program_id(0) == 0


def both(val):
    return val[:SUB] + val[SUB:]


def row_scales(x_ref, more=None):
    found = []
    for b in range(SUB):
        square = other = jnp.zeros((TILE, LANES), F32)
        for j, cols in lane_tiles():
            xf = x_ref[b, :, cols].astype(F32)
            square = square + xf * xf
            if more is not None:
                other = other + xf * more(b, j, cols)
        rstd = lax.rsqrt(jnp.sum(square, axis=-1, keepdims=True) * (1.0 / DM) + NORM_EPS)
        found.append((rstd, jnp.sum(other, axis=-1, keepdims=True) * (1.0 / DM)))
    return found


def norm_kernel(x_ref, gz_ref, sc_ref, n_ref, g_ref, gb_ref, sn_ref, sg_ref):
    @pl.when(first_step())
    def _():
        gb_ref[...] = jnp.zeros_like(gb_ref)

    rows = row_scales(x_ref)
    for j, cols in lane_tiles():
        scale = 1.0 + sc_ref[:, cols]
        total = gb_ref[:, cols]
        for b in range(SUB):
            gf = gz_ref[b, :, cols].astype(F32)
            total = total + both(gf)
            sn_ref[j, pl.ds(b, TILE, stride=SUB), :] = x_ref[b, :, cols].astype(F32) * rows[b][0] * scale
            sg_ref[j, pl.ds(b, TILE, stride=SUB), :] = gf
        gb_ref[:, cols] = total
        n_ref[:, cols] = sn_ref[j].astype(BF)
        g_ref[:, cols] = sg_ref[j].astype(BF)


ROW_BLOCK = pl.BlockSpec((SUB * TILE, DM), lambda i: (i, 0))


def norm_call(x, gz, scale):
    seq = seq_block(0)
    return row_call(norm_kernel, 60, (0, NBLK), (x, gz, scale), [seq, seq, ONE_ROW], [ROW_BLOCK, ROW_BLOCK, SUM_BLOCK],
                    [sds((ROWS, DM), BF), sds((ROWS, DM), BF), sds((SUB, DM), F32)], 2)


def z_kernel(acc_ref, x_ref, bo_ref, *refs):
    z_ref, sa_ref = refs[-2:]
    for j, cols in lane_tiles():
        sa_ref[j] = acc_ref[:, cols]
    for b in range(SUB):
        for j, cols in lane_tiles():
            z_ref[b, :, cols] = (x_ref[b, :, cols].astype(F32) + (sa_ref[j, pl.ds(b, TILE, stride=SUB), :] + bo_ref[:, cols])).astype(BF)


def z_call(blocks, acc, x, b_out, whole=None):
    seq = seq_block(blocks[0])
    return row_call(z_kernel, 40, blocks, (acc, x, b_out), [ROW_BLOCK, seq, ONE_ROW], seq, sds((GRP * SUB, TOK, DM), BF), 1, whole)


def proj_kernel(act_ref, w_ref, x_ref, bo_ref, z_ref, sa_ref):
    tok = x_ref.shape[1]
    for half in range(0, WIDE, CH):
        acc = lax.dot_general(act_ref[...], w_ref[half:half + CH], NT, preferred_element_type=F32)
        for j in range(CH // LANES):
            sa_ref[half // LANES + j] = acc[:, j * LANES:(j + 1) * LANES]
    for b in range(SUB):
        for j in range(WIDE // LANES):
            cols = slice(j * LANES, (j + 1) * LANES)
            out = x_ref[b, :, cols].astype(F32) + (sa_ref[j, pl.ds(b, tok, stride=SUB), :] + bo_ref[:, cols])
            z_ref[b, :, cols] = out.astype(BF)


def proj_call(rows, acts, weight, x, b_out):
    seq = pl.BlockSpec((SUB, TOK, WIDE), lambda n, m: (m, 0, n))
    return pl.pallas_call(
        proj_kernel, grid=(DM // WIDE, rows // GROWS),
        in_specs=[pl.BlockSpec((GROWS, DM), lambda n, m: (m, 0)), pl.BlockSpec((WIDE, DM), lambda n, m: (n, 0)), seq, pl.BlockSpec((1, WIDE), lambda n, m: (0, n))],
        out_specs=seq, out_shape=sds((GRP * SUB, TOK, DM), BF), scratch_shapes=[pltpu.VMEM((WIDE // LANES, GROWS, LANES), F32)],
        compiler_params=params(), cost_estimate=cost(130), name="proj_z")(acts, weight, x, b_out)


def gx_kernel(dn_ref, x_ref, gz_ref, sc_ref, *refs):
    gx_ref, gs_ref, sa_ref = refs[-3:]

    @pl.when(first_step())
    def _():
        gs_ref[...] = jnp.zeros_like(gs_ref)

    for j, cols in lane_tiles():
        sa_ref[j] = dn_ref[:, cols]

    def grad(b, j):
        return sa_ref[j, pl.ds(b, TILE, stride=SUB), :]

    rows = row_scales(x_ref, lambda b, j, cols: grad(b, j) * (1.0 + sc_ref[:, cols]))
    back = [rstd * rstd * rstd * mean for rstd, mean in rows]
    for j, cols in lane_tiles():
        scale = 1.0 + sc_ref[:, cols]
        total = gs_ref[:, cols]
        for b in range(SUB):
            xf = x_ref[b, :, cols].astype(F32)
            dn = grad(b, j) * rows[b][0]
            total = total + both(dn * xf)
            gx_ref[b, :, cols] = (gz_ref[b, :, cols].astype(F32) + (dn * scale - xf * back[b])).astype(BF)
        gs_ref[:, cols] = total


def gx_call(blocks, dn, x, gz, scale, whole=None):
    seq = seq_block(blocks[0])
    return row_call(gx_kernel, 50, blocks, (dn, x, gz, scale), [ROW_BLOCK, seq, seq, ONE_ROW], [seq, SUM_BLOCK],
                    [sds((GRP * SUB, TOK, DM), BF), sds((SUB, DM), F32)], 1, whole)


def run(steps):
    for _ in steps:
        pass


LAG_TAPS, LAG_GATES, LAG_GRADS, LAG_BACK, LAG_DX = 4, 5, 10, 11, 15
STRIPS = tuple(range(0, PIECE, STRIP))


def rnn_kernel(own, groups, units, chip_of, col_of, *refs):
    it = iter(refs)

    def take(count):
        return [next(it) for _ in range(count)]

    n_hbm, g_hbm = take(2)
    if own:
        own_w = take(3)
        gate_hbm = take(1)
    else:
        gate_hbm = take(2)
    par_ref, pos_ref = take(2)
    if not own:
        take(4)
    mixed_hbm, dyx_hbm, wyx_hbm, wz_hbm = take(4)
    outs = [mixed_hbm, dyx_hbm, dyx_hbm]
    if own:
        outs += take(3)
        conv_hbm, dpre_hbm, stat_ref = take(3)
    nbuf, gbuf, wbuf, wgf, wgb, py, dm, xbuf, ab, uv, yb, w1b, pb, qab, qib, mib, dbuf, conv, pre, dpre, dconv, st_m, st_y, st_x, st1, st2, enter, csend, crecv = take(29)
    if own:
        rb = next(it)
    if not own:
        stage = next(it)
    n_sem, g_sem, w_sem, wo_sem, wg_sem, o_sem, c_send, c_recv, d_send, d_recv, x_send, x_recv = take(12)
    if own:
        p_sem = next(it)

    core = lax.axis_index("cp")
    peer = 1 - core
    pieces = GROWS // PIECE
    steps = units * pieces
    xslots = xbuf.shape[0]
    share = 220 if own else 180

    def unit_of(q):
        return lax.div(q, pieces), lax.rem(q, pieces)

    def block_of(u):
        return lax.div(u, groups), lax.rem(u, groups)

    def al(val, mult=SUB):
        return pl.multiple_of(val, mult)

    def row_copy(q, which):
        u, i = unit_of(q)
        rows = pl.ds(al(block_of(u)[1] * GROWS + i * PIECE, PIECE), PIECE)
        slot = lax.rem(q, 2)
        src, dst, sem = ((n_hbm, nbuf, n_sem), (g_hbm, gbuf, g_sem))[which]
        return pltpu.make_async_copy(src.at[rows], dst.at[slot], sem.at[slot])

    blocks, turns = units // groups, groups * pieces

    def weight_in(blk, kind):
        slot = lax.rem(blk, 2)
        return pltpu.make_async_copy(own_w[kind].at[:, pl.ds(al(blk * CH, CH), CH)], wbuf.at[slot, kind], w_sem.at[slot, kind])

    def weight_out(blk, kind):
        slot = lax.rem(blk, 2)
        col = col_of(blk, True) * CH + (DM if kind == 1 else 0)
        dst = wz_hbm if kind == 2 else wyx_hbm
        return pltpu.make_async_copy(wbuf.at[slot, kind], dst.at[:, pl.ds(al(col, CH), CH)], wo_sem.at[slot, kind])

    per_half = 3 * HALF // WROWS

    def strip_slot(t, half):
        return lax.rem(t + half * per_half, DEPTH)

    def strip_in(blk, t, half):
        rows = pl.ds(al(t * WROWS, WROWS), WROWS)
        return pltpu.make_async_copy(gate_hbm[half].at[chip_of(blk)[0], rows], stage.at[strip_slot(t, half)], w_sem.at[strip_slot(t, half)])

    def strip_cast(blk, t, half):
        per_kind = HALF // WROWS
        row = (peer if half else core) * HALF + lax.rem(t, per_kind) * WROWS
        wbuf[lax.rem(blk, 2), lax.div(t, per_kind), pl.ds(al(row, WROWS), WROWS), :] = stage[strip_slot(t, half)].astype(BF)

    def weight_turn(q):
        blk, t = lax.div(q, turns), lax.rem(q, turns)

        @pl.when((t == 0) & (blk >= 1) & (blk + 1 < blocks))
        def _():
            for kind in range(3):
                weight_out(blk - 1, kind).wait()

        if own:
            @pl.when(t == 0)
            def _():
                for kind in range(3):
                    weight_in(blk, kind).wait()
                    weight_out(blk, kind).start()

                @pl.when(blk + 1 < blocks)
                def _():
                    for kind in range(3):
                        weight_in(blk + 1, kind).start()

            return
        more = blk + 1 < blocks
        for half in range(2):
            done = t - 1 - half * per_half

            @pl.when(more & (done >= 0) & (done < per_half))
            def _(half=half, done=done):
                strip_in(blk + 1, done, half).wait()
                strip_cast(blk + 1, done, half)
        for half in range(2):
            new = t - half * per_half

            @pl.when(more & (new >= 0) & (new < per_half))
            def _(half=half, new=new):
                strip_in(blk + 1, new, half).start()

        @pl.when(more & (t == 2 * per_half + 1))
        def _():
            for kind in range(3):
                weight_out(blk + 1, kind).start()

    def weights_first():
        if own:
            for kind in range(3):
                weight_in(0, kind).start()
            return
        ahead = DEPTH - 1
        for t in range(ahead):
            strip_in(0, t, 0).start()
        for half in range(2):
            def turn(t, _, half=half):
                @pl.when(t + ahead < per_half)
                def _():
                    strip_in(0, t + ahead, half).start()

                if half == 0:
                    @pl.when(t + ahead >= per_half)
                    def _():
                        strip_in(0, t + ahead - per_half, 1).start()
                strip_in(0, t, half).wait()
                strip_cast(0, t, half)
                return 0

            lax.fori_loop(0, per_half, turn, 0)
        for kind in range(3):
            weight_out(0, kind).start()

    def gate_copies(blk):
        slot = lax.rem(blk, 2)
        chip, j = chip_of(blk)
        if own:
            return [pltpu.make_async_copy(gate_hbm[0].at[j], wgf.at[slot], wg_sem.at[0, slot])]
        rows = pl.ds(3 * HALF, CH)
        return [pltpu.make_async_copy(gate_hbm[w].at[chip, rows], wgf.at[slot, (peer if w else core)], wg_sem.at[w, slot]) for w in range(2)]

    def out_copy(q, lag, which, forward):
        u, i = unit_of(q - lag)
        blk, grp = block_of(u)
        p = i if forward is None else i + forward * (pieces - 1 - 2 * i)
        slot = lax.rem(q, 2)
        src = (st_m, st_y, st_x)[which % 3].at[slot]
        rows = pl.ds(al(grp * GROWS + p * PIECE, PIECE), PIECE)
        col = blk if which >= 3 else col_of(blk, True) + (DM // CH if which == 2 else 0)
        return pltpu.make_async_copy(src, outs[which].at[rows, pl.ds(al(col * CH, CH), CH)], o_sem.at[which, slot])

    def conv_copy(q):
        u, i = unit_of(q - LAG_TAPS)
        blk, grp = block_of(u)
        p = i + core * (pieces - 1 - 2 * i)
        slot = lax.rem(q, 2)
        rows = pl.ds(al(grp * GROWS + p * PIECE, PIECE), PIECE)
        return pltpu.make_async_copy(conv.at[slot], conv_hbm.at[blk, rows], p_sem.at[0, slot])

    def dpre_copy(q):
        u, i = unit_of(q - LAG_GRADS)
        blk, grp = block_of(u)
        p = i + peer * (pieces - 1 - 2 * i)
        slot = lax.rem(q, 2)
        rows = pl.ds(al(grp * GROWS + p * PIECE, PIECE), PIECE)
        return pltpu.make_async_copy(dpre.at[slot], dpre_hbm.at[blk, rows], p_sem.at[1, slot])

    def remote(src, dst, send, recv):
        return pltpu.make_async_remote_copy(src_ref=src, dst_ref=dst, send_sem=send, recv_sem=recv, device_id={"cp": peer}, device_id_type=pl.DeviceIdType.MESH)

    def halo_copy(u):
        slot, sem = lax.rem(u, xslots), lax.rem(u, 2)
        return remote(xbuf.at[slot, pl.ds(HALO + GROWS - 24, 24)], xbuf.at[slot, pl.ds(HALO - 24, 24)], x_send.at[sem], x_recv.at[sem])

    def carry_copy(u):
        slot = lax.rem(u, 2)
        return remote(csend.at[slot], crecv.at[slot], c_send.at[slot], c_recv.at[slot])

    def dconv_copy(u):
        slot = lax.rem(u, 2)
        return remote(dbuf.at[slot, pl.ds(0, 24)], dbuf.at[slot, pl.ds(GROWS, 24)], d_send.at[slot], d_recv.at[slot])

    def out_copies(q):
        grads = (q >= LAG_GRADS) & (q < steps + LAG_GRADS)
        last = (q >= LAG_DX) & (q < steps + LAG_DX)
        made = []
        for which in range(len(outs)):
            lag, forward, when = (LAG_DX, None, last) if which % 3 == 2 else (LAG_GRADS, peer, grads)
            made.append((when, functools.partial(out_copy, q, lag, which, forward)))
        if own:
            made += [((q >= LAG_TAPS) & (q < steps + LAG_TAPS), lambda: conv_copy(q)), (grads, lambda: dpre_copy(q))]
        return made

    def at(q, lag, i):
        return (q >= lag) & (q < steps + lag) & (lax.rem(q - lag + pieces, pieces) == i)

    def rowpos(base, k):
        pos = pos_ref[pl.ds(al(base + k * SUB), STRIP), :]
        return jnp.concatenate([pos, pos], axis=1)

    def param(blk, k):
        chip, j = chip_of(blk)
        return par_ref[chip, j, k:k + 1, :]

    def stage_at(q, lag):
        u, i = unit_of(jnp.maximum(q - lag, 0))
        blk, grp = block_of(u)
        return u, i, blk, grp

    zero = lax.div(core, 2)

    def folded(val):
        return jnp.sum(val.reshape(STRIP // SUB, SUB, CH), axis=0)

    def scan_piece(slot, p, back, state):
        first = (p * (PIECE // SUB) + back * (PIECE // SUB - 1)) * SUB
        ahead, stride = first + SUB * back, SUB - 16 * back
        for tt in range(PIECE // SUB):
            decay = ab[slot, pl.ds(al(ahead + tt * stride), SUB), :]
            at_t = pl.ds(al(first + tt * stride + SUB), SUB)
            state = uv[back, slot, at_t, :] + decay * state
            uv[back, slot, at_t, :] = state
            yield 6
        return state

    def products(q):
        u, i, blk, _ = stage_at(q, 0)
        slot, w, us, xs = lax.rem(q, 2), lax.rem(blk, 2), lax.rem(u, 2), lax.rem(u, xslots)
        totals = []
        for src, kind in ((nbuf, 1), (nbuf, 0), (gbuf, 2)):
            total = None
            for k in range(0, DM, KSTEP):
                part = jnp.dot(src[slot, :, k:k + KSTEP], wbuf[w, kind, k:k + KSTEP], preferred_element_type=F32)
                total = part if total is None else total + part
                yield
            if kind == 1:
                total = (total + param(blk, 11)).astype(BF).astype(F32)
                xbuf[xs, pl.ds(al(i * PIECE + HALO), PIECE), :] = total
            totals.append(total)
        yield
        rows = pl.ds(al(i * PIECE, PIECE), PIECE)
        py[us, rows, :] = totals[1] + param(blk, 10)
        dm[us, rows, :] = totals[2]

    def taps(q):
        u, i, blk, grp = stage_at(q, LAG_TAPS)
        base = (i + core * (pieces - 1 - 2 * i)) * PIECE
        xs, cs = lax.rem(u, xslots), lax.rem(q, 2)
        par = [param(blk, k) for k in range(5)]
        for rt in STRIPS:
            pos = rowpos(grp * POS_ROWS + base + rt, 0)
            acc = par[0]
            for k in range(4):
                xk = xbuf[xs, pl.ds(al(base + rt + HALO - SUB * k), STRIP), :]
                if k:
                    xk = jnp.where(pos >= float(k), xk, 0.0)
                acc = acc + xk * par[1 + k]
            conv[cs, rt:rt + STRIP, :] = acc.astype(BF)
            yield 34
        pre[:PIECE] = jnp.dot(conv[cs], wgb[lax.rem(blk, 2)], preferred_element_type=F32)

    def gates(q):
        u, i, blk, grp = stage_at(q, LAG_GATES)
        p = i + core * (pieces - 1 - 2 * i)
        slot, cs = lax.rem(u, 2), lax.rem(q + 1, 2)
        base = p * PIECE
        ba, bi, kh = (param(blk, k) for k in range(5, SUB))
        for rt in STRIPS:
            rd = pl.ds(al(rt + zero * STRIP, STRIP), STRIP)
            rows = pl.ds(al(base + rt, STRIP), STRIP)
            rows8 = pl.ds(al(base + rt + SUB), STRIP)
            v = py[slot, rows, :]
            dmv = dm[slot, rows, :]
            v2 = v * v
            g = 0.5 * jnp.tanh(v * (v2 * GELU_K1 + GELU_K0)) + 0.5
            y = v * g
            yb[slot, rows, :] = y
            w1b[slot, rows, :] = dmv * (g + (v * (g - g * g)) * (v2 * (6.0 * GELU_K1) + 2.0 * GELU_K0))
            uv[1, slot, rows8, :] = dmv * y
            r2 = jnp.tanh(pre[rd, :CH] + ba) + 1.0
            thi = jnp.tanh(pre[rd, CH:] + bi)
            rate = jnp.where(rowpos(grp * POS_ROWS + base + rt, 0) < 0.5, FAR, r2 * kh)
            a = jnp.exp2(rate * -LOG2E)
            msq = jnp.tanh(rate) * (1.0 + a * a)
            rs = lax.rsqrt(jnp.maximum(msq, TINY))
            c = conv[cs, rt:rt + STRIP, :].astype(F32)
            gi = 0.5 * thi + 0.5
            mi = (msq * rs) * gi
            u_in = mi * c
            ab[slot, rows, :] = a
            mib[slot, rows, :] = mi
            uv[0, slot, rows8, :] = u_in
            pb[slot, rows, :] = (gi * c) * (a * rs)
            qab[slot, rows, :] = (a * rate) * (2.0 - r2)
            qib[slot, rows, :] = u_in * (1.0 - thi)
            if own:
                rb[slot, rows, :] = a * r2
            yield 112
        state = yield from scan_piece(slot, p, core, jnp.where(i == 0, 0.0, st1[...]))
        st1[...] = state
        csend[slot] = ab[slot, pl.ds(al(peer * GROWS), SUB), :] * state

    def grads(q):
        _, i, blk, _ = stage_at(q, LAG_GRADS)
        p = i + peer * (pieces - 1 - 2 * i)
        slot = lax.rem(lax.div(q + 3 * pieces - LAG_GRADS, pieces) + 1, 2)
        so = lax.rem(q, 2)
        base = p * PIECE
        entering = enter[...]
        uv[0, slot, pl.ds(0, SUB), :] = jnp.where(core == 1, entering, 0.0)
        st2[...] = yield from scan_piece(slot, p, peer, jnp.where(i == 0, entering, st2[...]))
        sums = [jnp.zeros((SUB, CH), F32)] * 4
        for rt in STRIPS:
            rl = slice(rt, rt + STRIP)
            rows = pl.ds(al(base + rt, STRIP), STRIP)
            rows8 = pl.ds(al(base + rt + SUB), STRIP)
            hid = uv[0, slot, rows8, :]
            dh = uv[1, slot, rows8, :]
            st_m[so, rl, :] = (hid * yb[slot, rows, :]).astype(BF)
            dpy = w1b[slot, rows, :] * hid
            st_y[so, rl, :] = dpy.astype(BF)
            g1 = dh * (pb[slot, rows, :] - uv[0, slot, rows, :])
            dpa = g1 * qab[slot, rows, :]
            dpi = dh * qib[slot, rows, :]
            dconv[rl, :] = dh * mib[slot, rows, :]
            dpre[so, rl, :CH] = dpa.astype(BF)
            dpre[so, rl, CH:] = dpi.astype(BF)
            if own:
                for k, val in enumerate((dpy, dpa, dpi, g1 * rb[slot, rows, :])):
                    sums[k] = sums[k] + folded(val)
            yield 56
        if own:
            for k in range(4):
                stat_ref[blk, k * SUB:k * SUB + SUB, :] += jnp.where(q >= LAG_GRADS, sums[k], 0.0)

    def back(q):
        u, i, blk, grp = stage_at(q, LAG_BACK)
        base = (i + peer * (pieces - 1 - 2 * i)) * PIECE
        slot, so = lax.rem(u, 2), lax.rem(q + 1, 2)
        xs = lax.rem(lax.div(jnp.maximum(q, LAG_BACK - pieces) - LAG_BACK + 4 * pieces, pieces), xslots)
        val = lax.dot_general(dpre[so], wgb[lax.rem(blk, 2)], NT, preferred_element_type=F32)
        dbuf[slot, pl.ds(al(base, PIECE), PIECE), :] = dconv[...] + val
        yield 60
        if own:
            sums = [jnp.zeros((SUB, CH), F32)] * 5
            for rt in STRIPS:
                pos = rowpos(grp * POS_ROWS + base + rt, 0)
                dc = dbuf[slot, pl.ds(al(base + rt, STRIP), STRIP), :]
                sums[0] = sums[0] + folded(dc)
                for k in range(4):
                    xk = xbuf[xs, pl.ds(al(base + rt + HALO - SUB * k), STRIP), :]
                    if k:
                        xk = jnp.where(pos >= float(k), xk, 0.0)
                    sums[1 + k] = sums[1 + k] + folded(dc * xk)
                yield 40
            for k in range(5):
                stat_ref[blk, (5 + k) * SUB:(5 + k) * SUB + SUB, :] += jnp.where(q >= LAG_BACK, sums[k], 0.0)

    def taps_back(q):
        u, i, blk, grp = stage_at(q, LAG_DX)
        slot, so = lax.rem(u, 2), lax.rem(q, 2)
        base = i * PIECE
        par = [param(blk, k) for k in range(1, 5)]
        total = jnp.zeros((SUB, CH), F32)
        for rt in STRIPS:
            acc = dbuf[slot, pl.ds(al(base + rt), STRIP), :] * par[0]
            for k in range(1, 4):
                dk = dbuf[slot, pl.ds(al(base + rt + SUB * k), STRIP), :]
                acc = acc + jnp.where(rowpos(grp * POS_ROWS + base + rt, k) >= float(k), dk, 0.0) * par[k]
            st_x[so, rt:rt + STRIP, :] = acc.astype(BF)
            if own:
                total = total + folded(acc)
            yield 32
        if own:
            stat_ref[blk, 32:40, :] += jnp.where(q >= LAG_DX, total, 0.0)

    def start_of_step(q):
        for when, make in out_copies(q - 2):
            @pl.when(when)
            def _(make=make):
                make().wait()

        @pl.when(at(q, LAG_TAPS, 3) & (core == 0))
        def _():
            halo_copy(lax.div(q - LAG_TAPS, pieces)).wait_send()

        @pl.when(at(q, LAG_TAPS, 3) & (core == 1))
        def _():
            halo_copy(lax.div(q - LAG_TAPS, pieces)).wait_recv()

        @pl.when(at(q, LAG_GRADS, 0))
        def _():
            u = lax.div(q - LAG_GRADS, pieces)
            carry_copy(u).wait()
            enter[...] = crecv[lax.rem(u, 2)]

        @pl.when(at(q, LAG_DX, 3))
        def _():
            dconv_copy(lax.div(q - LAG_DX, pieces)).wait()

        @pl.when((q >= LAG_TAPS) & (q < steps + LAG_TAPS) & (lax.rem(q - LAG_TAPS + groups * pieces, groups * pieces) == 0))
        def _():
            blk = lax.div(q - LAG_TAPS, groups * pieces)
            for cp in gate_copies(blk):
                cp.wait()
            slot = lax.rem(blk, 2)
            wgb[slot, :, :CH] = wgf[slot, 0].astype(BF)
            wgb[slot, :, CH:] = wgf[slot, 1].astype(BF)

            @pl.when(blk + 1 < blocks)
            def _():
                for cp in gate_copies(blk + 1):
                    cp.start()

    def end_of_step(q):
        for when, make in out_copies(q):
            @pl.when(when)
            def _(make=make):
                make().start()

        @pl.when(at(q, LAG_TAPS, 0) & (core == 0))
        def _():
            halo_copy(lax.div(q - LAG_TAPS, pieces)).start()

        @pl.when(at(q, LAG_GATES, 3))
        def _():
            carry_copy(lax.div(q - LAG_GATES, pieces)).start()

        @pl.when(at(q, LAG_BACK, 3))
        def _():
            dconv_copy(lax.div(q - LAG_BACK, pieces)).start()

    for which in range(2):
        row_copy(0, which).start()
    for cp in gate_copies(0):
        cp.start()
    weights_first()
    for slot in range(2):
        ab[slot, pl.ds(GROWS, SUB), :] = jnp.ones((SUB, CH), F32)
    if own:
        stat_ref[...] = jnp.zeros_like(stat_ref)
    barrier = pltpu.get_barrier_semaphore()
    pl.semaphore_signal(barrier, inc=1, device_id={"cp": peer}, device_id_type=pl.DeviceIdType.MESH)
    pl.semaphore_wait(barrier, 1)

    def full_step(q, _):
        for which in range(2):
            row_copy(q, which).wait()

        @pl.when(q + 1 < steps)
        def _():
            for which in range(2):
                row_copy(q + 1, which).start()

        weight_turn(q)
        start_of_step(q)
        product_steps, spent, made = products(q), share, 0
        for stage in (taps_back, back, grads, gates, taps):
            for bundles in stage(q):
                spent += bundles
                while spent >= share and made < 3 * DM // KSTEP:
                    spent -= share
                    made += 1
                    next(product_steps)
        run(product_steps)
        end_of_step(q)
        return 0

    lax.fori_loop(0, steps, full_step, 0)

    def drain_step(q, _):
        start_of_step(q)
        for lag, stage in ((LAG_DX, taps_back), (LAG_BACK, back), (LAG_GRADS, grads), (LAG_GATES, gates), (LAG_TAPS, taps)):
            @pl.when(q < steps + lag)
            def _(stage=stage):
                run(stage(q))
        end_of_step(q)
        return 0

    lax.fori_loop(steps, steps + LAG_DX, drain_step, 0)
    for blk in (blocks - 2, blocks - 1):
        for kind in range(3):
            weight_out(jnp.int32(blk), kind).wait()
    for q in (steps + LAG_DX, steps + LAG_DX + 1):
        for when, make in out_copies(jnp.int32(q - 2)):
            @pl.when(when)
            def _(make=make):
                make().wait()


def rnn_call(phase, groups, n, gz, sources, par, pos, whole):
    own = phase is None
    units = (4 if own else 3) * groups

    def chip_of(blk):
        return (0, blk) if own else (lax.rem(lax.axis_index("tp") + 1 + blk, 4), 0)

    def col_of(blk, merged):
        return lax.axis_index("tp") * 4 + blk if own else chip_of(blk)[0] * 4 + phase

    args = [n, gz, *sources, par, pos, *whole]
    in_specs = [ANY] * (2 + len(sources)) + [VM] * 2 + [ANY] * len(whole)
    out_specs = [ANY] * 4
    out_shape = [sds((ROWS, DM), BF), sds((ROWS, 2 * DM), BF), sds((DM, 2 * DM), BF), sds((DM, DM), BF)]
    alias = {6 + k: k for k in range(len(whole))}
    if own:
        out_specs = [ANY] * 9 + [VM]
        out_shape = out_shape + [sds((ROWS, 4 * CH), BF)] * 3 + [sds((4, ROWS, CH), BF), sds((4, ROWS, 2 * CH), BF), sds((4, 10 * SUB, CH), F32)]

    def buf(slots, rows, dtype=F32, cols=CH):
        return pltpu.VMEM((slots, rows, cols), dtype)

    piece32 = pltpu.VMEM((PIECE, CH), F32)
    scratch = [buf(2, PIECE, BF, DM), buf(2, PIECE, BF, DM), pltpu.VMEM((2, 3, DM, CH), BF), pltpu.VMEM((2, 2, CH, CH), F32), buf(2, CH, BF, 2 * CH),
               buf(2, GROWS), buf(2, GROWS), buf(4 if own else 2, GROWS + HALO), buf(2, GROWS + SUB),
               pltpu.VMEM((2, 2, GROWS + SUB, CH), F32)] + [buf(2, GROWS)] * 6 + [buf(2, GROWS + HALO), buf(2, PIECE, BF),
               pltpu.VMEM((PIECE + STRIP, 2 * CH), F32), buf(2, PIECE, BF, 2 * CH), piece32] + [buf(2, PIECE, BF)] * 3 + [pltpu.VMEM((SUB, CH), F32)] * 3 + [buf(2, SUB)] * 2
    dma = pltpu.SemaphoreType.DMA
    sems = [dma((2,)), dma((2,)), dma((2, 3) if own else (DEPTH,)), dma((2, 3)), dma((2, 2)), dma((6 if own else 3, 2))] + [dma((2,))] * 6
    if own:
        scratch.append(buf(2, GROWS))
        sems.append(dma((2, 2)))
    else:
        scratch.append(buf(DEPTH, WROWS))
    return pl.pallas_call(
        functools.partial(rnn_kernel, own, groups, units, chip_of, col_of), in_specs=in_specs, out_specs=out_specs, out_shape=out_shape,
        scratch_shapes=scratch + sems, input_output_aliases=alias,
        compiler_params=params(collective_id=0 if own else 1 + phase, has_side_effects=True),
        cost_estimate=cost(10 * units))(*args)


def layer(x_in, grad_z, seg_pos, norm_scale, w_x, b_x, w_y, b_y, conv_w, conv_b, w_a, b_a, w_i, b_i, a_param, w_out, b_out):
    core = lax.axis_index("cp")
    swap = [(0, 1), (1, 0)]
    half = core * HALF

    zero = jnp.zeros_like(a_param)
    rows = [conv_b.astype(F32)] + [conv_w[k].astype(F32) for k in range(4)] + [0.5 * b_a.astype(F32), 0.5 * b_i.astype(F32), 4.0 * jax.nn.softplus(a_param), zero, zero,
            b_y.astype(F32), b_x.astype(F32)] + [zero] * 4
    par_own = jnp.stack(rows).reshape(16, 4, CH).transpose(1, 0, 2)
    wg_own = jnp.stack([w_a, w_i], axis=1).astype(F32) * 0.5
    wg_mine = lax.dynamic_index_in_dim(wg_own, core, 1, keepdims=False)

    got = []
    for j in range(4):
        cols = j * CH
        rows_out = lax.dynamic_slice(w_out, (cols, half), (CH, HALF))
        if j == 0:
            rows_out = lax.optimization_barrier(rows_out)
        parts = [lax.dynamic_slice(w_y, (half, cols), (HALF, CH)).astype(F32), lax.dynamic_slice(w_x, (half, cols), (HALF, CH)).astype(F32),
                 rows_out.T.astype(F32), wg_mine[j], par_own[j]]
        mine = lax.optimization_barrier(jnp.concatenate(parts, axis=0))
        got.append(lax.all_gather(mine, "tp"))

    def partner(val):
        return lax.ppermute(val, "cp", swap)

    pos = seg_pos.astype(jnp.int32)
    later = jnp.where(core == 0, partner(pos[:, :SUB]), -1)
    pos = jnp.concatenate([pos, later], axis=1).reshape(GRP, SUB, TOK + SUB).transpose(0, 2, 1).astype(F32)
    pos = jnp.broadcast_to(pos.reshape(GRP * POS_ROWS, 1), (GRP * POS_ROWS, LANES))

    scale = norm_scale.astype(F32)[None]
    n, gz, gb = norm_call(x_in, grad_z, scale)

    first = rnn_call(None, GRP, n, gz, (w_y, w_x, w_out.T, wg_own), par_own[None], pos, ())
    whole, (omixed, ody, odx, conv16, dpre16, stats) = first[:4], first[4:]

    def dot(lhs, rhs, dims):
        return lax.dot_general(lhs, rhs, dims, preferred_element_type=F32)

    for j in range(4):
        other = partner(got[j])
        whole = rnn_call(j, GRP, n, gz, (got[j], other), got[j][:, None, 3 * HALF + CH:], pos, whole)
    mixed, dyx, wyx, wz = whole

    g_w_x = dot(n, odx, TN)
    g_w_y = dot(n, ody, TN)
    g_w_out = dot(omixed, gz, TN)
    g_gate = 0.5 * jnp.einsum("hrk,hrj->hkj", conv16, dpre16, preferred_element_type=F32)
    stats = jnp.sum(stats.reshape(4, 10, SUB, CH), axis=2).transpose(1, 0, 2).reshape(10, 4 * CH)

    def merged(val):
        theirs = partner(val)
        return val + theirs

    g_w_x, g_w_y, g_w_out, g_gate = merged(g_w_x), merged(g_w_y), merged(g_w_out), merged(g_gate)

    def shared(acts, weight, full):
        own_rows = (ROWS - full) // 4
        mine = lax.dynamic_slice(acts, (full + lax.axis_index("tp") * own_rows, 0), (own_rows, acts.shape[1]))
        mine = lax.optimization_barrier(dot(mine, weight, NT))
        return lax.all_gather(mine, "tp", tiled=True)

    bias = b_out.astype(F32)[None]
    dn_mid, z_mid = FULL_DN // (SUB * TILE), FULL_Z // (SUB * TILE)
    dn_rest, z_rest = shared(dyx, wyx, FULL_DN), shared(mixed, wz, FULL_Z)
    grad_x, gs = gx_call((0, dn_mid), dot(dyx[:FULL_DN], wyx, NT), x_in, grad_z, scale)
    grad_x, gs_rest = gx_call((dn_mid, NBLK), dn_rest, x_in, grad_z, scale, grad_x)
    gs = gs + gs_rest
    z_out = proj_call(FULL_Z, mixed, wz, x_in, bias)
    z_out = z_call((z_mid, NBLK), z_rest, x_in, bias, z_out)

    sums = jnp.concatenate([jnp.sum(gs, axis=0), stats.reshape(-1), jnp.sum(gb, axis=0)])
    sums = merged(sums)
    g_scale, stats, g_b_out = sums[:DM], sums[DM:-DM].reshape(10, 4 * CH), sums[-DM:]
    return (z_out, grad_x, g_scale, g_w_x, stats[4], g_w_y, stats[0], stats[6:10], stats[5], g_gate[:, :, :CH], 0.5 * stats[1],
            g_gate[:, :, CH:], 0.5 * stats[2], 4.0 * jax.nn.sigmoid(a_param) * stats[3], g_w_out, g_b_out)


def solution(mesh):
    return jax.shard_map(layer, mesh=mesh, in_specs=IN_SPECS, out_specs=OUT_SPECS, check_vma=False)
```
